32 devices in a mesh: grp: 4 (over z), shard: 8 (over y, x, core).
Axes of the slice: x: 2, y: 2, z: 4, core: 2. Of those that a mesh axis runs over, the one named last changes fastest.
Arguments:
- partial_grads: bfloat16 [4, 4096, 6144], P('grp', 'shard')
- joined_block: int32 [48], replicated, may hold values from 0 to 47, each once
- head_slot: int32 [48], replicated, may hold values from 0 to 47, as said below
Outputs:
- head_grads: float32 [48, 8, 512, 128], P('shard', None, 'grp')
- head_rms: float32 [48], P('shard')
- type_rms: float32 [3], replicated
The draws below stay inside these ranges and needn't reach their ends.
Inputs may be any that keep to these rules, and one draw needn't show every extreme that they name: `joined_block`: a permutation: each block number appears once. `head_slot`: distinct slots; every owner along shard holds 6 or 5 head blocks, and some owner holds 6.
All inputs are finite; a program needn't handle non-finite values.
Results may differ from the reference program's by a relative error of at most 0.0003.
Values may be sent and summed in bfloat16 or wider, within the bound.
A program may use at most 64 MiB of HBM per device.

```python
import jax
import jax.numpy as jnp
from jax import lax

D = 4096
QH = 32
KVH = 8
HS = 128
BLOCKS = 48
COLS = 6144
SLOTS_DEV = 6
SLOTS = 48
N_GRP = 4
N_SHARD = 8


def draw_partial_grads(key, part):
    row_index = jnp.arange(D)
    block_pos = (row_index % (D // N_SHARD)).astype(jnp.float32) / (D // N_SHARD)
    rise = jnp.exp(jnp.log(3.0) * block_pos)
    row_scale = jnp.exp(jax.random.uniform(jax.random.fold_in(key, 11), (D,), jnp.float32, 0.0, jnp.log(10.0))) * rise
    col_scale = jnp.exp(jax.random.uniform(jax.random.fold_in(key, 12), (COLS,), jnp.float32, 0.0, jnp.log(10.0)))
    overall = 0.01

    def draw_group(group):
        noise = jax.random.normal(jax.random.fold_in(jax.random.fold_in(key, 14), group), (D, COLS), jnp.float32)
        return (noise * row_scale[:, None] * col_scale[None, :] * overall).astype(jnp.bfloat16)
    return lax.map(draw_group, jnp.arange(N_GRP))


def draw_head_slot(key, part):
    slot_total = SLOTS_DEV * N_SHARD
    empty_count = slot_total - BLOCKS
    owners = jax.random.permutation(jax.random.fold_in(key, 21), N_SHARD).astype(jnp.int32)
    lost_pos = jax.random.randint(jax.random.fold_in(key, 22), (N_SHARD,), 0, SLOTS_DEV).astype(jnp.int32)
    lost_slot = owners * SLOTS_DEV + lost_pos
    chosen = jnp.arange(N_SHARD, dtype=jnp.int32) < empty_count
    slot_ids = jnp.arange(slot_total, dtype=jnp.int32)
    dead_slot = jnp.any((slot_ids[:, None] == lost_slot[None, :]) & chosen[None, :], axis=1)
    sort_keys = dead_slot.astype(jnp.int32) * slot_total + slot_ids
    live_slots = jnp.argsort(sort_keys).astype(jnp.int32)[:BLOCKS]
    shuffle = jax.random.permutation(jax.random.fold_in(key, 23), BLOCKS).astype(jnp.int32)
    return live_slots[shuffle].astype(jnp.int32)


def setup_inputs(seed: int = 0) -> dict:
    streams_of = jax.random.split(jax.random.key(seed), 4)
    return {
        "partial_grads": draw_partial_grads(jax.random.fold_in(streams_of[3], 71), 0),
        "joined_block": jax.random.permutation(streams_of[1], BLOCKS).astype(jnp.int32),
        "head_slot": draw_head_slot(jax.random.fold_in(streams_of[3], 71), 0),
    }


def reference(partial_grads, joined_block, head_slot):

    def add_group(carry, group_term):
        return (carry + group_term.astype(jnp.float32), None)
    reduced, _ = lax.scan(add_group, jnp.zeros((D, COLS), jnp.float32), partial_grads)
    block_ids = jnp.arange(BLOCKS, dtype=jnp.int32)
    block_kind = (block_ids >= QH).astype(jnp.int32) + (block_ids >= QH + KVH).astype(jnp.int32)
    matches = (head_slot[None, :] == jnp.arange(SLOTS, dtype=jnp.int32)[:, None]).astype(jnp.int32)
    occupied = lax.optimization_barrier(jnp.sum(matches, axis=1))
    source = lax.optimization_barrier(jnp.sum(matches * joined_block[None, :], axis=1)).astype(jnp.int32)
    slot_kind = lax.optimization_barrier(jnp.sum(matches * block_kind[None, :], axis=1)) + (1 - occupied) * 3
    picked = jnp.take(reduced.reshape(D, BLOCKS, HS), source, axis=1)
    picked = picked * occupied.astype(jnp.float32)[None, :, None]
    head_grads = jnp.transpose(picked, (1, 0, 2)).reshape(SLOTS, N_SHARD, D // N_SHARD, HS)
    squares = lax.optimization_barrier(jnp.sum(head_grads * head_grads, axis=(1, 2, 3)))
    head_rms = jnp.sqrt(squares / (D * HS))
    selector = (slot_kind[:, None] == jnp.arange(3, dtype=jnp.int32)[None, :]).astype(jnp.float32)
    type_squares = lax.optimization_barrier(jnp.sum(squares[:, None] * selector, axis=0))
    counts = jnp.array([QH, KVH, KVH], jnp.float32) * (D * HS)
    type_rms = jnp.sqrt(type_squares / counts)
    return (head_grads, head_rms, type_rms)
```

```python
import functools

import jax
import jax.numpy as jnp
from jax import lax
from jax.experimental import pallas as pl
from jax.experimental.pallas import tpu as pltpu
from jax.sharding import PartitionSpec as P

D = 4096
QH = 32
KVH = 8
HS = 128
LANES = 128
MESH = pl.DeviceIdType.MESH


def chunk_rows(rows):
    return 16 if rows % 16 == 0 else rows


PART = 8
GROUP = 8
QMAX = 524286.0
SMALL = 2.0**-64
PLAN = (("RRM", 8), ("M", 8))


def encode(tiles):
    peak = functools.reduce(jnp.maximum, [jnp.abs(t) for t in tiles])
    peak = jnp.max(peak, axis=0, keepdims=True)
    lift = jnp.where(peak < SMALL, 1.0 / SMALL, 1.0)
    scale = QMAX / jnp.maximum(peak * lift, SMALL)
    codes = [jnp.round(t * lift * scale).astype(jnp.int32) for t in tiles]
    half = GROUP // 2
    words = [(codes[i] << 12) | (codes[half + i] & 4095) for i in range(half)]
    tops = [((codes[half + i] >> 12) & 255) << (8 * i) for i in range(half)]
    words.append(functools.reduce(jnp.bitwise_or, tops))
    return words, peak


def decode(words, peak):
    half = GROUP // 2
    codes = [words[i] >> 12 for i in range(half)]
    for i in range(half):
        top = (words[half] << (24 - 8 * i)) >> 24
        codes.append((top << 12) | (words[i] & 4095))
    return [c.astype(jnp.float32) * (1.0 / QMAX) * peak for c in codes]


def flip(s, o):
    for b in range(3):
        if o >> b & 1:
            s = s + (1 - 2 * lax.rem(lax.div(s, 1 << b), 2)) * (1 << b)
    return s


def line_kernel(
    blocks,
    slots_dev,
    x_ref,
    joined_ref,
    slot_ref,
    out_ref,
    head_ref,
    type_ref,
    own,
    far,
    passed,
    got,
    out_words,
    out_peaks,
    in_words,
    in_peaks,
    ready,
    source,
    taken,
    kind_of,
    summed,
    squares,
    grp_part,
    grp_all,
    shard_part,
    shard_all,
    own_sem,
    far_sem,
    plane_sem,
    beyond_sem,
    r_send,
    r_recv,
    m_send,
    m_recv,
    w_send,
    w_recv,
    p_send,
    p_recv,
    a_send,
    a_recv,
    keep_sem,
    g_send,
    g_recv,
    s_send,
    s_recv,
):
    groups, shards = 4, 8
    grp = lax.axis_index("grp")
    shard = lax.axis_index("shard")
    slots = slots_dev * shards
    chunks = own.shape[0]
    width = own.shape[2] // blocks
    sets = blocks // GROUP
    span = GROUP * width

    outer = (grp == 0) | (grp == groups - 1)
    inner = jnp.logical_not(outer)
    mate = grp + 1 - 2 * lax.rem(grp, 2)
    near = jnp.where(outer, 3 - mate, 3 - grp)
    beyond = near + 1 - 2 * lax.rem(near, 2)
    dests = (near, beyond)

    own_copy = pltpu.make_async_copy(x_ref.at[pl.ds(grp * chunks, chunks)], own, own_sem)

    def far_copy(f):
        return pltpu.make_async_copy(
            x_ref.at[pl.ds(dests[f] * chunks, chunks)], far.at[f], far_sem.at[f]
        )

    def send(src, dst, send_sem, recv_sem, to):
        return pltpu.make_async_remote_copy(
            src_ref=src,
            dst_ref=dst,
            send_sem=send_sem,
            recv_sem=recv_sem,
            device_id=to,
            device_id_type=MESH,
        )

    def relay_copy(c, f):
        src = x_ref.at[dests[f] * chunks + c]
        return send(src, passed.at[c, f], r_send.at[c, f], r_recv.at[c, f], (mate, shard))

    def mate_copy(c):
        src = x_ref.at[mate * chunks + c]
        return send(src, got.at[c], m_send.at[c], m_recv.at[c], (mate, shard))

    def coded_copies(c, f):
        to = (dests[f], shard)
        return (
            send(out_words.at[c, f], in_words.at[c], w_send.at[c, f], w_recv.at[c], to),
            send(out_peaks.at[c, f], in_peaks.at[c], p_send.at[c, f], p_recv.at[c], to),
        )

    order = (6, 7, 2, 4, 3, 5, 1)

    def rows_copy(c, o):
        to = flip(shard, o)
        return send(
            ready.at[c, pl.ds(to * slots_dev, slots_dev)],
            out_ref.at[:, shard, pl.ds(pl.multiple_of(c * PART, PART), PART), :],
            a_send.at[c, o - 1],
            a_recv.at[c, o - 1],
            (grp, to),
        )

    def keep_copy(c):
        return pltpu.make_async_copy(
            ready.at[c, pl.ds(shard * slots_dev, slots_dev)],
            out_ref.at[:, shard, pl.ds(pl.multiple_of(c * PART, PART), PART), :],
            keep_sem.at[c],
        )

    def settle(c):
        for o in order:
            rows_copy(c, o).wait()
        keep_copy(c).wait()

    own_copy.start()

    barrier = pltpu.get_barrier_semaphore()
    pl.semaphore_signal(barrier, 1, device_id=(mate, shard), device_id_type=MESH)
    for o in range(1, 6):
        pl.semaphore_signal(barrier, 1, device_id=(grp, flip(shard, o)), device_id_type=MESH)

    @pl.when(inner)
    def _():
        pl.semaphore_signal(barrier, 1, device_id=(near, shard), device_id_type=MESH)
        pl.semaphore_wait(barrier, 7)
        pl.semaphore_signal(beyond_sem, 1, device_id=(near, shard), device_id_type=MESH)
        for f in range(2):
            far_copy(f).start()

    @pl.when(outer)
    def _():
        pl.semaphore_wait(barrier, 6)
        r = m = 0
        for pattern, times in PLAN:
            nr, nm = pattern.count("R"), pattern.count("M")

            def queue(k, carry, pattern=pattern, r=r, m=m, nr=nr, nm=nm):
                i = j = 0
                for kind in pattern:
                    if kind == "R":
                        for f in range(2):
                            relay_copy(r + k * nr + i, f).start()
                        i += 1
                    else:
                        mate_copy(m + k * nm + j).start()
                        j += 1
                return carry

            lax.fori_loop(0, times, queue, 0)
            r, m = r + times * nr, m + times * nm

    pl.semaphore_signal(plane_sem, 1, device_id=(grp, flip(shard, 2)), device_id_type=MESH)

    def find(j, carry):
        head = jnp.int32(-1)
        for b in range(blocks):
            head = jnp.where(slot_ref[b] == j, b, head)
        there = head >= 0
        source[j] = jnp.where(there, joined_ref[jnp.maximum(head, 0)], 0)
        taken[j] = jnp.where(there, 1.0, 0.0)
        kind = jnp.where(head >= QH, 1, 0) + jnp.where(head >= QH + KVH, 1, 0)
        kind_of[j] = jnp.where(there, kind, 3)
        return carry

    lax.fori_loop(0, slots, find, 0)
    own_copy.wait()

    def clear(j, carry):
        squares[j] = jnp.zeros((PART, width), jnp.float32)
        return carry

    lax.fori_loop(0, slots, clear, 0)

    def pack(c):
        mate_copy(c).start()
        for f in range(2):
            relay_copy(c, f).wait_recv()

            def pack_set(p, carry, f=f):
                at = pl.ds(pl.multiple_of(p * span, span), span)
                total = far[f, c, :, at].astype(jnp.float32) + passed[c, f, :, at].astype(jnp.float32)
                words, peak = encode([total[:, i * width : (i + 1) * width] for i in range(GROUP)])
                for i, word in enumerate(words):
                    out_words[c, f, p, i] = word
                out_peaks[c, f, p] = peak
                return carry

            lax.fori_loop(0, sets, pack_set, 0, unroll=2)
            for copy in coded_copies(c, f):
                copy.start()

    def finish(c):
        for copy in coded_copies(c, 0):
            copy.wait_recv()

        def pre_set(p, carry):
            at = pl.ds(pl.multiple_of(p * span, span), span)
            mine = own[c, :, at].astype(jnp.float32)
            tiles = decode([in_words[c, p, i] for i in range(GROUP // 2 + 1)], in_peaks[c, p])
            for i, tile in enumerate(tiles):
                summed[p * GROUP + i] = mine[:, i * width : (i + 1) * width] + tile
            return carry

        lax.fori_loop(0, sets, pre_set, 0, unroll=2)
        mate_copy(c).wait_recv()

        def add_set(p, carry):
            at = pl.ds(pl.multiple_of(p * span, span), span)
            more = got[c, :, at].astype(jnp.float32)
            for i in range(GROUP):
                summed[p * GROUP + i] += more[:, i * width : (i + 1) * width]
            return carry

        lax.fori_loop(0, sets, add_set, 0, unroll=2)

        def place(j, carry):
            total = summed[source[j]] * taken[j]
            ready[c, j] = total
            squares[j] += total * total
            return carry

        lax.fori_loop(0, slots, place, 0, unroll=8)
        for o in order:
            rows_copy(c, o).start()
        keep_copy(c).start()

    LAG = 3

    def finish_and_settle(c, carry=0):
        finish(c)

        @pl.when(c >= LAG)
        def _():
            settle(c - LAG)

        return carry

    @pl.when(inner)
    def _():
        for f in range(2):
            far_copy(f).wait()
        pl.semaphore_wait(beyond_sem, 1)
        pl.semaphore_wait(plane_sem, 1)
        r = m = 0
        for pattern, times in PLAN:
            nr, nm = pattern.count("R"), pattern.count("M")

            def act(k, carry, pattern=pattern, r=r, m=m, nr=nr, nm=nm):
                i = j = 0
                for kind in pattern:
                    if kind == "R":
                        pack(r + k * nr + i)
                        i += 1
                    else:
                        finish_and_settle(m + k * nm + j)
                        j += 1
                return carry

            lax.fori_loop(0, times, act, 0)
            r, m = r + times * nr, m + times * nm

    @pl.when(outer)
    def _():
        pl.semaphore_wait(plane_sem, 1)
        lax.fori_loop(0, chunks, finish_and_settle, 0)

    lane = lax.broadcasted_iota(jnp.int32, (slots, LANES), 1)
    row = lax.broadcasted_iota(jnp.int32, (slots, LANES), 0)
    per_slot = jnp.sum(jnp.sum(squares[...], axis=1), axis=1, keepdims=True)
    total = jnp.sum(jnp.where(lane == row, per_slot, 0.0), axis=0, keepdims=True)

    def grp_copy(o):
        to = lax.rem(grp + o, groups)
        return send(grp_part, grp_all.at[o - 1], g_send.at[o - 1], g_recv.at[o - 1], (to, shard))

    def shard_copy(o):
        to = flip(shard, o)
        return send(
            shard_part, shard_all.at[o - 1], s_send.at[o - 1], s_recv.at[o - 1], (grp, to)
        )

    grp_part[...] = total
    for o in range(1, groups):
        grp_copy(o).start()
    lane = lax.broadcasted_iota(jnp.int32, (1, LANES), 1)

    def lay(j, kinds):
        return jnp.where(lane == j, kind_of[j], kinds)

    kinds = lax.fori_loop(0, slots, lay, jnp.full((1, LANES), 3, jnp.int32))

    @pl.when(inner)
    def _():
        def drain(c, carry):
            mate_copy(c).wait_send()
            for f in range(2):
                for copy in coded_copies(c, f):
                    copy.wait_send()
            return carry

        lax.fori_loop(0, chunks, drain, 0)

    @pl.when(outer)
    def _():
        def drain(c, carry):
            mate_copy(c).wait_send()
            for f in range(2):
                relay_copy(c, f).wait_send()
            return carry

        lax.fori_loop(0, chunks, drain, 0)

    for o in range(1, groups):
        grp_copy(o).wait()
        total = total + grp_all[o - 1]
    shard_part[...] = total
    for o in order:
        shard_copy(o).start()
    for c in range(chunks - LAG, chunks):
        settle(c)
    for o in order:
        shard_copy(o).wait()
        total = total + shard_all[o - 1]
    root = jnp.sqrt(total / (D * HS))
    for i in range(slots_dev):
        head_ref[i] = jnp.sum(jnp.where(lane == shard * slots_dev + i, root, 0.0))
    for t, heads in enumerate((QH, KVH, KVH)):
        one = jnp.sum(jnp.where(kinds == t, total, 0.0), axis=1, keepdims=True)
        type_ref[t] = jnp.sum(jnp.sqrt(one / (heads * D * HS)))


def line_step(x, joined, slot, blocks, slots_dev, shards, rows, width):
    chunks = rows // PART
    cols = blocks * width
    sets = blocks // GROUP
    slots = slots_dev * shards
    half = GROUP // 2
    dma = pltpu.SemaphoreType.DMA
    regular = pltpu.SemaphoreType.REGULAR
    f32, i32, bf16 = jnp.float32, jnp.int32, jnp.bfloat16
    return pl.pallas_call(
        functools.partial(line_kernel, blocks, slots_dev),
        out_shape=[
            pltpu.VMEM((slots_dev, shards, rows, width), f32),
            jax.ShapeDtypeStruct((slots_dev,), f32),
            jax.ShapeDtypeStruct((3,), f32),
        ],
        in_specs=[
            pl.BlockSpec(memory_space=pltpu.HBM),
            pl.BlockSpec(memory_space=pltpu.SMEM),
            pl.BlockSpec(memory_space=pltpu.SMEM),
        ],
        out_specs=[
            pl.BlockSpec(memory_space=pltpu.VMEM),
            pl.BlockSpec(memory_space=pltpu.SMEM),
            pl.BlockSpec(memory_space=pltpu.SMEM),
        ],
        scratch_shapes=[
            pltpu.VMEM((chunks, PART, cols), bf16),
            pltpu.VMEM((2, chunks, PART, cols), bf16),
            pltpu.VMEM((chunks, 2, PART, cols), bf16),
            pltpu.VMEM((chunks, PART, cols), bf16),
            pltpu.VMEM((chunks, 2, sets, half + 1, PART, width), i32),
            pltpu.VMEM((chunks, 2, sets, 1, width), f32),
            pltpu.VMEM((chunks, sets, half + 1, PART, width), i32),
            pltpu.VMEM((chunks, sets, 1, width), f32),
            pltpu.VMEM((chunks, slots, PART, width), f32),
            pltpu.SMEM((slots,), i32),
            pltpu.SMEM((slots,), f32),
            pltpu.SMEM((slots,), i32),
            pltpu.VMEM((blocks, PART, width), f32),
            pltpu.VMEM((slots, PART, width), f32),
            pltpu.VMEM((1, LANES), f32),
            pltpu.VMEM((3, 1, LANES), f32),
            pltpu.VMEM((1, LANES), f32),
            pltpu.VMEM((shards - 1, 1, LANES), f32),
            dma,
            dma((2,)),
            regular,
            regular,
            dma((chunks, 2)),
            dma((chunks, 2)),
            dma((chunks,)),
            dma((chunks,)),
            dma((chunks, 2)),
            dma((chunks,)),
            dma((chunks, 2)),
            dma((chunks,)),
            dma((chunks, shards - 1)),
            dma((chunks, shards - 1)),
            dma((chunks,)),
            dma((3,)),
            dma((3,)),
            dma((shards - 1,)),
            dma((shards - 1,)),
        ],
        compiler_params=pltpu.CompilerParams(
            collective_id=0,
            has_side_effects=True,
            vmem_limit_bytes=57 * 1024 * 1024,
        ),
    )(x.reshape(4 * chunks, PART, cols), joined, slot)


def any_kernel(groups, shards, blocks, slots_dev, chunks, *refs):
    x_ref, joined_ref, slot_ref = refs[:3]
    out_ref, head_ref, type_ref = refs[3:6]
    own = refs[6]
    got = refs[7 : 7 + chunks]
    ready = refs[7 + chunks : 7 + 2 * chunks]
    rest = refs[7 + 2 * chunks :]
    (source, taken, kind_of, summed, squares, shard_part, shard_all, grp_part, grp_all) = rest[:9]
    (own_sem, z_send, z_recv, a_send, a_recv, keep_sem, s_send, s_recv, g_send, g_recv) = rest[9:]

    grp = lax.axis_index("grp")
    shard = lax.axis_index("shard")
    slots = slots_dev * shards
    rows = own.shape[0]
    part = rows // chunks
    width = own.shape[1] // blocks

    def grp_peer(offset):
        return lax.rem(grp + offset, groups)

    def shard_peer(offset):
        return lax.rem(shard + offset, shards)

    load_own = pltpu.make_async_copy(
        x_ref.at[0, pl.ds(pl.multiple_of(grp * rows, 8), rows), :], own, own_sem
    )
    load_own.start()

    barrier = pltpu.get_barrier_semaphore()
    for o in range(1, groups):
        pl.semaphore_signal(barrier, 1, device_id=(grp_peer(o), shard), device_id_type=MESH)
    for o in range(1, shards):
        pl.semaphore_signal(barrier, 1, device_id=(grp, shard_peer(o)), device_id_type=MESH)
    pl.semaphore_wait(barrier, groups + shards - 2)

    z_copies = []
    for c in range(chunks):
        for o in range(1, groups):
            first = pl.multiple_of(grp_peer(o) * rows + c * part, 8)
            copy = pltpu.make_async_remote_copy(
                src_ref=x_ref.at[0, pl.ds(first, part), :],
                dst_ref=got[c].at[o - 1],
                send_sem=z_send.at[c, o - 1],
                recv_sem=z_recv.at[c, o - 1],
                device_id=(grp_peer(o), shard),
                device_id_type=MESH,
            )
            copy.start()
            z_copies.append(copy)

    def find(j, carry):
        found, block, kind = jnp.float32(0), jnp.int32(0), jnp.int32(3)
        for b in range(blocks):
            hit = slot_ref[b] == j
            found = jnp.where(hit, 1.0, found)
            block = jnp.where(hit, joined_ref[b], block)
            kind = jnp.where(hit, (b >= QH) + (b >= QH + KVH), kind)
        source[j] = block
        taken[j] = found
        kind_of[j] = kind
        return carry

    lax.fori_loop(0, slots, find, 0)

    load_own.wait()
    a_copies = []
    for c in range(chunks):
        for o in range(1, groups):
            z_copies[c * (groups - 1) + o - 1].wait_recv()

        def add(k, carry):
            at = pl.multiple_of(k * width, width)
            total = own[c * part : (c + 1) * part, pl.ds(at, width)].astype(jnp.float32)
            for o in range(1, groups):
                total += got[c][o - 1, :, pl.ds(at, width)].astype(jnp.float32)
            summed[k] = total
            return carry

        lax.fori_loop(0, blocks, add, 0, unroll=4)

        def slot(j, carry):
            total = summed[source[j]] * taken[j]
            ready[c][j] = total
            sq = jnp.sum((total * total).reshape(part // 8, 8, width), axis=0)
            squares[j] = sq if c == 0 else squares[j] + sq
            return carry

        lax.fori_loop(0, slots, slot, 0, unroll=4)

        if c == chunks - 1:
            lane = lax.broadcasted_iota(jnp.int32, (slots, LANES), 1)
            row = lax.broadcasted_iota(jnp.int32, (slots, LANES), 0)
            per_slot = jnp.sum(jnp.sum(squares[...], axis=1), axis=1, keepdims=True)
            shard_part[...] = jnp.sum(jnp.where(lane == row, per_slot, 0.0), axis=0, keepdims=True)
            s_copies = []
            for o in range(1, shards):
                copy = pltpu.make_async_remote_copy(
                    src_ref=shard_part,
                    dst_ref=shard_all.at[o - 1],
                    send_sem=s_send.at[o - 1],
                    recv_sem=s_recv.at[o - 1],
                    device_id=(grp, shard_peer(o)),
                    device_id_type=MESH,
                )
                copy.start()
                s_copies.append(copy)

        for o in range(1, shards):
            copy = pltpu.make_async_remote_copy(
                src_ref=ready[c].at[pl.ds(shard_peer(o) * slots_dev, slots_dev)],
                dst_ref=out_ref.at[:, shard, pl.ds(c * part, part), :],
                send_sem=a_send.at[c, o - 1],
                recv_sem=a_recv.at[c, o - 1],
                device_id=(grp, shard_peer(o)),
                device_id_type=MESH,
            )
            copy.start()
            a_copies.append(copy)
        copy = pltpu.make_async_copy(
            ready[c].at[pl.ds(shard * slots_dev, slots_dev)],
            out_ref.at[:, shard, pl.ds(c * part, part), :],
            keep_sem.at[c],
        )
        copy.start()
        a_copies.append(copy)

    total = shard_part[...]
    for o in range(1, shards):
        s_copies[o - 1].wait()
        total = total + shard_all[o - 1]
    grp_part[...] = total
    g_copies = []
    for o in range(1, groups):
        copy = pltpu.make_async_remote_copy(
            src_ref=grp_part,
            dst_ref=grp_all.at[o - 1],
            send_sem=g_send.at[o - 1],
            recv_sem=g_recv.at[o - 1],
            device_id=(grp_peer(o), shard),
            device_id_type=MESH,
        )
        copy.start()
        g_copies.append(copy)
    lane = lax.broadcasted_iota(jnp.int32, (1, LANES), 1)

    def lay(j, kinds):
        return jnp.where(lane == j, kind_of[j], kinds)

    kinds = lax.fori_loop(0, slots, lay, jnp.full((1, LANES), 3, jnp.int32))
    for o in range(1, groups):
        g_copies[o - 1].wait()
        total = total + grp_all[o - 1]
    root = jnp.sqrt(total / (D * HS))
    for i in range(slots_dev):
        head_ref[i] = jnp.sum(jnp.where(lane == shard * slots_dev + i, root, 0.0))
    for t, heads in enumerate((QH, KVH, KVH)):
        one = jnp.sum(jnp.where(kinds == t, total, 0.0), axis=1, keepdims=True)
        type_ref[t] = jnp.sum(jnp.sqrt(one / (heads * D * HS)))

    for copy in z_copies:
        copy.wait_send()
    for copy in a_copies:
        copy.wait()


def any_step(x, joined, slot, groups, shards, blocks, slots_dev, rows, width):
    slots = slots_dev * shards
    cols = blocks * width
    part = chunk_rows(rows)
    chunks = rows // part
    dma = pltpu.SemaphoreType.DMA
    return pl.pallas_call(
        functools.partial(any_kernel, groups, shards, blocks, slots_dev, chunks),
        out_shape=[
            jax.ShapeDtypeStruct((slots_dev, shards, rows, width), jnp.float32),
            jax.ShapeDtypeStruct((slots_dev,), jnp.float32),
            jax.ShapeDtypeStruct((3,), jnp.float32),
        ],
        in_specs=[
            pl.BlockSpec(memory_space=pltpu.HBM),
            pl.BlockSpec(memory_space=pltpu.SMEM),
            pl.BlockSpec(memory_space=pltpu.SMEM),
        ],
        out_specs=[
            pl.BlockSpec(memory_space=pl.ANY),
            pl.BlockSpec(memory_space=pltpu.SMEM),
            pl.BlockSpec(memory_space=pltpu.SMEM),
        ],
        scratch_shapes=[pltpu.VMEM((rows, cols), jnp.bfloat16)]
        + [pltpu.VMEM((groups - 1, part, cols), jnp.bfloat16)] * chunks
        + [pltpu.VMEM((slots, part, width), jnp.float32)] * chunks
        + [
            pltpu.SMEM((slots,), jnp.int32),
            pltpu.SMEM((slots,), jnp.float32),
            pltpu.SMEM((slots,), jnp.int32),
            pltpu.VMEM((blocks, part, width), jnp.float32),
            pltpu.VMEM((slots, 8, width), jnp.float32),
            pltpu.VMEM((1, LANES), jnp.float32),
            pltpu.VMEM((shards - 1, 1, LANES), jnp.float32),
            pltpu.VMEM((1, LANES), jnp.float32),
            pltpu.VMEM((groups - 1, 1, LANES), jnp.float32),
            dma,
            dma((chunks, groups - 1)),
            dma((chunks, groups - 1)),
            dma((chunks, shards - 1)),
            dma((chunks, shards - 1)),
            dma((chunks,)),
            dma((shards - 1,)),
            dma((shards - 1,)),
            dma((groups - 1,)),
            dma((groups - 1,)),
        ],
        compiler_params=pltpu.CompilerParams(
            collective_id=0,
            has_side_effects=True,
            vmem_limit_bytes=60 * 1024 * 1024,
        ),
    )(x, joined, slot)


def solution(mesh):
    groups, shards = mesh.shape["grp"], mesh.shape["shard"]

    def step(x, joined, slot):
        blocks = joined.shape[0]
        slots_dev = (blocks + shards - 1) // shards
        rows = x.shape[1] // groups
        width = x.shape[2] // blocks
        line = groups == 4 and shards == 8 and rows == 16 * PART and blocks % GROUP == 0
        if line and width == LANES and slots_dev * shards <= LANES:
            return tuple(line_step(x, joined, slot, blocks, slots_dev, shards, rows, width))
        return tuple(any_step(x, joined, slot, groups, shards, blocks, slots_dev, rows, width))

    return jax.shard_map(
        step,
        mesh=mesh,
        in_specs=(P("grp", "shard", None), P(), P()),
        out_specs=(P("shard", None, "grp", None), P("shard"), P()),
        check_vma=False,
    )
```

```python
import functools

import jax
import jax.numpy as jnp
from jax import lax
from jax.experimental import pallas as pl
from jax.experimental.pallas import tpu as pltpu
from jax.sharding import PartitionSpec as P

D = 4096
QH = 32
KVH = 8
HS = 128
LANES = 128
MESH = pl.DeviceIdType.MESH


def chunk_rows(rows):
    return 16 if rows % 16 == 0 else rows


PART = 8
GROUP = 8
QMAX = 524286.0
SMALL = 2.0**-64
LATE = 3
PLAN = (("FNFNLFNLFNFNLFNMA", 1), ("FNFNM", 5), ("M", 7))
HOLD = 2
AHEAD = 4
LAG = 3


def encode(tiles):
    peak = functools.reduce(jnp.maximum, [jnp.abs(t) for t in tiles])
    peak = jnp.max(peak, axis=0, keepdims=True)
    lift = jnp.where(peak < SMALL, 1.0 / SMALL, 1.0)
    scale = QMAX / jnp.maximum(peak * lift, SMALL)
    codes = [jnp.round(t * lift * scale).astype(jnp.int32) for t in tiles]
    half = GROUP // 2
    words = [(codes[i] << 12) | (codes[half + i] & 4095) for i in range(half)]
    tops = [((codes[half + i] >> 12) & 255) << (8 * i) for i in range(half)]
    words.append(functools.reduce(jnp.bitwise_or, tops))
    return words, peak


def decode(words, peak):
    half = GROUP // 2
    codes = [words[i] >> 12 for i in range(half)]
    for i in range(half):
        top = (words[half] << (24 - 8 * i)) >> 24
        codes.append((top << 12) | (words[i] & 4095))
    return [c.astype(jnp.float32) * (1.0 / QMAX) * peak for c in codes]


def flip(s, o):
    for b in range(3):
        if o >> b & 1:
            s = s + (1 - 2 * lax.rem(lax.div(s, 1 << b), 2)) * (1 << b)
    return s


def line_kernel(
    blocks,
    slots_dev,
    x_ref,
    joined_ref,
    slot_ref,
    out_ref,
    head_ref,
    type_ref,
    own,
    far,
    passed,
    got,
    out_words,
    out_peaks,
    in_words,
    in_peaks,
    ready,
    late_src,
    late_mine,
    late_in,
    late_raw,
    late_words,
    late_peaks,
    back_words,
    back_peaks,
    source,
    taken,
    kind_of,
    summed,
    squares,
    grp_part,
    grp_all,
    shard_part,
    shard_all,
    own_sem,
    far_sem,
    plane_sem,
    beyond_sem,
    r_send,
    r_recv,
    m_send,
    m_recv,
    w_send,
    w_recv,
    p_send,
    p_recv,
    a_send,
    a_recv,
    keep_sem,
    g_send,
    g_recv,
    s_send,
    s_recv,
    late_sem,
    lx_send,
    lx_recv,
    lk_sem,
    lf_send,
    lf_recv,
    la_send,
    la_recv,
):
    groups, shards = 4, 8
    grp = lax.axis_index("grp")
    shard = lax.axis_index("shard")
    slots = slots_dev * shards
    chunks = own.shape[0]
    width = own.shape[2] // blocks
    sets = blocks // GROUP
    span = GROUP * width

    outer = (grp == 0) | (grp == groups - 1)
    inner = jnp.logical_not(outer)
    mate = grp + 1 - 2 * lax.rem(grp, 2)
    near = jnp.where(outer, 3 - mate, 3 - grp)
    beyond = near + 1 - 2 * lax.rem(near, 2)
    dests = (near, beyond)

    own_copy = pltpu.make_async_copy(x_ref.at[pl.ds(grp * chunks, chunks)], own, own_sem)

    def far_copy(f):
        return pltpu.make_async_copy(
            x_ref.at[pl.ds(dests[f] * chunks, chunks)], far.at[f], far_sem.at[f]
        )

    def send(src, dst, send_sem, recv_sem, to):
        return pltpu.make_async_remote_copy(
            src_ref=src,
            dst_ref=dst,
            send_sem=send_sem,
            recv_sem=recv_sem,
            device_id=to,
            device_id_type=MESH,
        )

    def relay_copy(c, f):
        src = x_ref.at[dests[f] * chunks + c]
        return send(src, passed.at[c, f], r_send.at[c, f], r_recv.at[c, f], (mate, shard))

    def mate_copy(c):
        src = x_ref.at[mate * chunks + c]
        return send(src, got.at[c], m_send.at[c], m_recv.at[c], (mate, shard))

    def coded_copies(c, f):
        to = (dests[f], shard)
        return (
            send(out_words.at[c, f], in_words.at[c], w_send.at[c, f], w_recv.at[c], to),
            send(out_peaks.at[c, f], in_peaks.at[c], p_send.at[c, f], p_recv.at[c], to),
        )

    order = (6, 7, 2, 4, 3, 5, 1)

    def rows_copy(c, o):
        to = flip(shard, o)
        return send(
            ready.at[c, pl.ds(to * slots_dev, slots_dev)],
            out_ref.at[:, shard, pl.ds(pl.multiple_of(c * PART, PART), PART), :],
            a_send.at[c, o - 1],
            a_recv.at[c, o - 1],
            (grp, to),
        )

    def keep_copy(c):
        return pltpu.make_async_copy(
            ready.at[c, pl.ds(shard * slots_dev, slots_dev)],
            out_ref.at[:, shard, pl.ds(pl.multiple_of(c * PART, PART), PART), :],
            keep_sem.at[c],
        )

    def settle(c):
        for o in order:
            rows_copy(c, o).wait()
        keep_copy(c).wait()

    late_copy = pltpu.make_async_copy(x_ref.at[pl.ds(mate * chunks, LATE)], late_src, late_sem)

    def swap_copy(o):
        to = flip(shard, o)
        return send(
            late_mine.at[:, pl.ds(to * slots_dev, slots_dev)],
            late_in.at[shard],
            lx_send.at[o - 1],
            lx_recv.at[o - 1],
            (grp, to),
        )

    stay_copy = pltpu.make_async_copy(
        late_mine.at[:, pl.ds(shard * slots_dev, slots_dev)], late_in.at[shard], lk_sem
    )

    def forward_copy(n):
        to = (mate, shard)
        return send(late_in.at[:, n], late_raw.at[:, n], lf_send.at[n], lf_recv.at[n], to)

    def back_copies():
        to = (mate, shard)
        return (
            send(late_words, back_words, la_send.at[0], la_recv.at[0], to),
            send(late_peaks, back_peaks, la_send.at[1], la_recv.at[1], to),
        )

    own_copy.start()

    barrier = pltpu.get_barrier_semaphore()
    pl.semaphore_signal(barrier, 1, device_id=(mate, shard), device_id_type=MESH)
    for o in range(1, 6):
        pl.semaphore_signal(barrier, 1, device_id=(grp, flip(shard, o)), device_id_type=MESH)

    @pl.when(inner)
    def _():
        pl.semaphore_signal(barrier, 1, device_id=(near, shard), device_id_type=MESH)
        pl.semaphore_wait(barrier, 7)
        pl.semaphore_signal(beyond_sem, 1, device_id=(near, shard), device_id_type=MESH)
        for f in range(2):
            far_copy(f).start()
        for c in range(AHEAD):
            mate_copy(c).start()

    @pl.when(outer)
    def _():
        pl.semaphore_wait(barrier, 6)
        done = dict(N=0, F=0, M=LATE)
        for pattern, times in PLAN:
            now, per = dict(done), {k: pattern.count(k) for k in done}

            def queue(k, carry, pattern=pattern, now=now, per=per):
                at = {key: now[key] + k * per[key] for key in now}
                for kind in pattern:
                    if kind in "NF":
                        relay_copy(at[kind], "NF".index(kind)).start()
                    elif kind == "M":
                        mate_copy(at[kind]).start()
                    if kind in at:
                        at[kind] += 1
                return carry

            lax.fori_loop(0, times, queue, 0)
            done = {key: now[key] + times * per[key] for key in now}
        late_copy.start()

    pl.semaphore_signal(plane_sem, 1, device_id=(grp, flip(shard, 2)), device_id_type=MESH)

    def find(j, carry):
        head = jnp.int32(-1)
        for b in range(blocks):
            head = jnp.where(slot_ref[b] == j, b, head)
        there = head >= 0
        source[j] = jnp.where(there, joined_ref[jnp.maximum(head, 0)], 0)
        taken[j] = jnp.where(there, 1.0, 0.0)
        kind = jnp.where(head >= QH, 1, 0) + jnp.where(head >= QH + KVH, 1, 0)
        kind_of[j] = jnp.where(there, kind, 3)
        return carry

    lax.fori_loop(0, slots, find, 0)
    own_copy.wait()

    def clear(j, carry):
        squares[j] = jnp.zeros((PART, width), jnp.float32)
        return carry

    lax.fori_loop(0, slots, clear, 0)

    def pack(c, f):
        relay_copy(c, f).wait_recv()

        def pack_set(p, carry):
            at = pl.ds(pl.multiple_of(p * span, span), span)
            total = far[f, c, :, at].astype(jnp.float32) + passed[c, f, :, at].astype(jnp.float32)
            words, peak = encode([total[:, i * width : (i + 1) * width] for i in range(GROUP)])
            for i, word in enumerate(words):
                out_words[c, f, p, i] = word
            out_peaks[c, f, p] = peak
            return carry

        lax.fori_loop(0, sets, pack_set, 0, unroll=2)
        for copy in coded_copies(c, f):
            copy.start()
        if f == 1:

            @pl.when(c + AHEAD < chunks)
            def _():
                mate_copy(c + AHEAD).start()

    def finish(c, late=False):
        for copy in coded_copies(c, 0):
            copy.wait_recv()

        def pre_set(p, carry):
            at = pl.ds(pl.multiple_of(p * span, span), span)
            mine = own[c, :, at].astype(jnp.float32)
            tiles = decode([in_words[c, p, i] for i in range(GROUP // 2 + 1)], in_peaks[c, p])
            for i, tile in enumerate(tiles):
                summed[p * GROUP + i] = mine[:, i * width : (i + 1) * width] + tile
            return carry

        lax.fori_loop(0, sets, pre_set, 0, unroll=2)
        if not late:
            mate_copy(c).wait_recv()

        def add_set(p, carry):
            at = pl.ds(pl.multiple_of(p * span, span), span)
            more = got[c, :, at].astype(jnp.float32)
            for i in range(GROUP):
                summed[p * GROUP + i] += more[:, i * width : (i + 1) * width]
            return carry

        if not late:
            lax.fori_loop(0, sets, add_set, 0, unroll=2)

        def place(j, carry):
            total = summed[source[j]] * taken[j]
            ready[c, j] = total
            if not late:
                squares[j] += total * total
            return carry

        lax.fori_loop(0, slots, place, 0, unroll=8)
        for o in order:
            rows_copy(c, o).start()
        keep_copy(c).start()

    def tell(j, carry):
        for n in range(LATE):
            at = pl.ds(n * PART, PART)
            words, peak = encode([out_ref[j, a, at, :] for a in range(shards)])
            for i, word in enumerate(words):
                late_words[n, j, i] = word
            late_peaks[n, j] = peak
        return carry

    def finish_and_settle(c, carry=0, first=0):
        finish(c)

        @pl.when(c >= first + LAG)
        def _():
            settle(c - LAG)

        return carry

    @pl.when(inner)
    def _():
        for f in range(2):
            far_copy(f).wait()
        pl.semaphore_wait(beyond_sem, 1)
        pl.semaphore_wait(plane_sem, 1)
        done = dict(N=0, F=0, L=0, M=LATE)
        for pattern, times in PLAN:
            now, per = dict(done), {k: pattern.count(k) for k in done}

            def act(k, carry, pattern=pattern, now=now, per=per):
                at = {key: now[key] + k * per[key] for key in now}
                for kind in pattern:
                    if kind in "NF":
                        pack(at[kind], "NF".index(kind))
                    elif kind == "M":
                        finish_and_settle(at[kind], first=LATE)
                    elif kind == "L":
                        finish(at[kind], late=True)
                    else:
                        for c in range(LATE):
                            settle(c)
                        lax.fori_loop(0, slots_dev, tell, 0)
                        for copy in back_copies():
                            copy.start()
                    if kind in at:
                        at[kind] += 1
                return carry

            lax.fori_loop(0, times, act, 0)
            done = {key: now[key] + times * per[key] for key in now}

    @pl.when(outer)
    def _():
        pl.semaphore_wait(plane_sem, 1)
        late_copy.wait()

        for n in range(LATE):

            def split(p, carry, n=n):
                at = pl.ds(pl.multiple_of(p * span, span), span)
                rows = late_src[n, :, at].astype(jnp.float32)
                for i in range(GROUP):
                    summed[p * GROUP + i] = rows[:, i * width : (i + 1) * width]
                return carry

            lax.fori_loop(0, sets, split, 0, unroll=2)

            def arrange(j, carry, n=n):
                late_mine[n, j] = (summed[source[j]] * taken[j]).astype(jnp.bfloat16)
                return carry

            lax.fori_loop(0, slots, arrange, 0, unroll=4)
        for o in order:
            swap_copy(o).start()
        stay_copy.start()
        for o in order:
            swap_copy(o).wait()
        stay_copy.wait()
        for n in range(LATE - HOLD):
            forward_copy(n).start()
        lax.fori_loop(0, chunks - LAG, finish_and_settle, 0)
        for copy in back_copies():
            copy.wait_recv()

        def late_squares(j, carry):
            acc = jnp.zeros((PART, width), jnp.float32)
            for n in range(LATE):
                tiles = decode([back_words[n, j, i] for i in range(GROUP // 2 + 1)], back_peaks[n, j])
                for a, tile in enumerate(tiles):
                    total = tile + late_in[a, n, j].astype(jnp.float32)
                    acc += total * total
            squares[shard * slots_dev + j] += acc
            return carry

        lax.fori_loop(0, slots_dev, late_squares, 0)
        lax.fori_loop(chunks - LAG, chunks, finish_and_settle, 0)

    lane = lax.broadcasted_iota(jnp.int32, (slots, LANES), 1)
    row = lax.broadcasted_iota(jnp.int32, (slots, LANES), 0)
    per_slot = jnp.sum(jnp.sum(squares[...], axis=1), axis=1, keepdims=True)
    total = jnp.sum(jnp.where(lane == row, per_slot, 0.0), axis=0, keepdims=True)

    def grp_copy(o):
        to = lax.rem(grp + o, groups)
        return send(grp_part, grp_all.at[o - 1], g_send.at[o - 1], g_recv.at[o - 1], (to, shard))

    def shard_copy(o):
        to = flip(shard, o)
        return send(
            shard_part, shard_all.at[o - 1], s_send.at[o - 1], s_recv.at[o - 1], (grp, to)
        )

    grp_part[...] = total
    for o in range(1, groups):
        grp_copy(o).start()

    @pl.when(outer)
    def _():
        for n in range(LATE - HOLD, LATE):
            forward_copy(n).start()

    lane = lax.broadcasted_iota(jnp.int32, (1, LANES), 1)

    def lay(j, kinds):
        return jnp.where(lane == j, kind_of[j], kinds)

    kinds = lax.fori_loop(0, slots, lay, jnp.full((1, LANES), 3, jnp.int32))

    @pl.when(inner)
    def _():
        def drain(c, carry):
            mate_copy(c).wait_send()
            for f in range(2):
                for copy in coded_copies(c, f):
                    copy.wait_send()
            return carry

        lax.fori_loop(0, chunks, drain, 0)
        for copy in back_copies():
            copy.wait_send()

    @pl.when(outer)
    def _():
        def drain(c, carry):
            for f in range(2):
                relay_copy(c, f).wait_send()

            @pl.when(c >= LATE)
            def _():
                mate_copy(c).wait_send()

            return carry

        lax.fori_loop(0, chunks, drain, 0)

    for o in range(1, groups):
        grp_copy(o).wait()
        total = total + grp_all[o - 1]
    shard_part[...] = total
    for o in order:
        shard_copy(o).start()
    for c in range(chunks - LAG, chunks):
        settle(c)
    for o in order:
        shard_copy(o).wait()
        total = total + shard_all[o - 1]
    root = jnp.sqrt(total / (D * HS))
    for i in range(slots_dev):
        head_ref[i] = jnp.sum(jnp.where(lane == shard * slots_dev + i, root, 0.0))
    for t, heads in enumerate((QH, KVH, KVH)):
        one = jnp.sum(jnp.where(kinds == t, total, 0.0), axis=1, keepdims=True)
        type_ref[t] = jnp.sum(jnp.sqrt(one / (heads * D * HS)))

    @pl.when(outer)
    def _():
        for n in range(LATE):
            forward_copy(n).wait_send()

    @pl.when(inner)
    def _():
        for n in range(LATE):
            forward_copy(n).wait_recv()

            def add_late(a, carry, n=n):
                for j in range(slots_dev):
                    at = pl.ds(n * PART, PART)
                    out_ref[j, a, at, :] += late_raw[a, n, j].astype(jnp.float32)
                return carry

            lax.fori_loop(0, shards, add_late, 0, unroll=True)


def line_step(x, joined, slot, blocks, slots_dev, shards, rows, width):
    chunks = rows // PART
    cols = blocks * width
    sets = blocks // GROUP
    slots = slots_dev * shards
    half = GROUP // 2
    dma = pltpu.SemaphoreType.DMA
    regular = pltpu.SemaphoreType.REGULAR
    f32, i32, bf16 = jnp.float32, jnp.int32, jnp.bfloat16
    return pl.pallas_call(
        functools.partial(line_kernel, blocks, slots_dev),
        out_shape=[
            pltpu.VMEM((slots_dev, shards, rows, width), f32),
            jax.ShapeDtypeStruct((slots_dev,), f32),
            jax.ShapeDtypeStruct((3,), f32),
        ],
        in_specs=[
            pl.BlockSpec(memory_space=pltpu.HBM),
            pl.BlockSpec(memory_space=pltpu.SMEM),
            pl.BlockSpec(memory_space=pltpu.SMEM),
        ],
        out_specs=[
            pl.BlockSpec(memory_space=pltpu.VMEM),
            pl.BlockSpec(memory_space=pltpu.SMEM),
            pl.BlockSpec(memory_space=pltpu.SMEM),
        ],
        scratch_shapes=[
            pltpu.VMEM((chunks, PART, cols), bf16),
            pltpu.VMEM((2, chunks, PART, cols), bf16),
            pltpu.VMEM((chunks, 2, PART, cols), bf16),
            pltpu.VMEM((chunks, PART, cols), bf16),
            pltpu.VMEM((chunks, 2, sets, half + 1, PART, width), i32),
            pltpu.VMEM((chunks, 2, sets, 1, width), f32),
            pltpu.VMEM((chunks, sets, half + 1, PART, width), i32),
            pltpu.VMEM((chunks, sets, 1, width), f32),
            pltpu.VMEM((chunks, slots, PART, width), f32),
            pltpu.VMEM((LATE, PART, cols), bf16),
            pltpu.VMEM((LATE, slots, PART, width), bf16),
            pltpu.VMEM((shards, LATE, slots_dev, PART, width), bf16),
            pltpu.VMEM((shards, LATE, slots_dev, PART, width), bf16),
            pltpu.VMEM((LATE, slots_dev, half + 1, PART, width), i32),
            pltpu.VMEM((LATE, slots_dev, 1, width), f32),
            pltpu.VMEM((LATE, slots_dev, half + 1, PART, width), i32),
            pltpu.VMEM((LATE, slots_dev, 1, width), f32),
            pltpu.SMEM((slots,), i32),
            pltpu.SMEM((slots,), f32),
            pltpu.SMEM((slots,), i32),
            pltpu.VMEM((blocks, PART, width), f32),
            pltpu.VMEM((slots, PART, width), f32),
            pltpu.VMEM((1, LANES), f32),
            pltpu.VMEM((3, 1, LANES), f32),
            pltpu.VMEM((1, LANES), f32),
            pltpu.VMEM((shards - 1, 1, LANES), f32),
            dma,
            dma((2,)),
            regular,
            regular,
            dma((chunks, 2)),
            dma((chunks, 2)),
            dma((chunks,)),
            dma((chunks,)),
            dma((chunks, 2)),
            dma((chunks,)),
            dma((chunks, 2)),
            dma((chunks,)),
            dma((chunks, shards - 1)),
            dma((chunks, shards - 1)),
            dma((chunks,)),
            dma((3,)),
            dma((3,)),
            dma((shards - 1,)),
            dma((shards - 1,)),
            dma,
            dma((shards - 1,)),
            dma((shards - 1,)),
            dma,
            dma((LATE,)),
            dma((LATE,)),
            dma((2,)),
            dma((2,)),
        ],
        compiler_params=pltpu.CompilerParams(
            collective_id=0,
            has_side_effects=True,
            vmem_limit_bytes=57 * 1024 * 1024,
        ),
    )(x.reshape(4 * chunks, PART, cols), joined, slot)


def any_kernel(groups, shards, blocks, slots_dev, chunks, *refs):
    x_ref, joined_ref, slot_ref = refs[:3]
    out_ref, head_ref, type_ref = refs[3:6]
    own = refs[6]
    got = refs[7 : 7 + chunks]
    ready = refs[7 + chunks : 7 + 2 * chunks]
    rest = refs[7 + 2 * chunks :]
    (source, taken, kind_of, summed, squares, shard_part, shard_all, grp_part, grp_all) = rest[:9]
    (own_sem, z_send, z_recv, a_send, a_recv, keep_sem, s_send, s_recv, g_send, g_recv) = rest[9:]

    grp = lax.axis_index("grp")
    shard = lax.axis_index("shard")
    slots = slots_dev * shards
    rows = own.shape[0]
    part = rows // chunks
    width = own.shape[1] // blocks

    def grp_peer(offset):
        return lax.rem(grp + offset, groups)

    def shard_peer(offset):
        return lax.rem(shard + offset, shards)

    load_own = pltpu.make_async_copy(
        x_ref.at[0, pl.ds(pl.multiple_of(grp * rows, 8), rows), :], own, own_sem
    )
    load_own.start()

    barrier = pltpu.get_barrier_semaphore()
    for o in range(1, groups):
        pl.semaphore_signal(barrier, 1, device_id=(grp_peer(o), shard), device_id_type=MESH)
    for o in range(1, shards):
        pl.semaphore_signal(barrier, 1, device_id=(grp, shard_peer(o)), device_id_type=MESH)
    pl.semaphore_wait(barrier, groups + shards - 2)

    z_copies = []
    for c in range(chunks):
        for o in range(1, groups):
            first = pl.multiple_of(grp_peer(o) * rows + c * part, 8)
            copy = pltpu.make_async_remote_copy(
                src_ref=x_ref.at[0, pl.ds(first, part), :],
                dst_ref=got[c].at[o - 1],
                send_sem=z_send.at[c, o - 1],
                recv_sem=z_recv.at[c, o - 1],
                device_id=(grp_peer(o), shard),
                device_id_type=MESH,
            )
            copy.start()
            z_copies.append(copy)

    def find(j, carry):
        found, block, kind = jnp.float32(0), jnp.int32(0), jnp.int32(3)
        for b in range(blocks):
            hit = slot_ref[b] == j
            found = jnp.where(hit, 1.0, found)
            block = jnp.where(hit, joined_ref[b], block)
            kind = jnp.where(hit, (b >= QH) + (b >= QH + KVH), kind)
        source[j] = block
        taken[j] = found
        kind_of[j] = kind
        return carry

    lax.fori_loop(0, slots, find, 0)

    load_own.wait()
    a_copies = []
    for c in range(chunks):
        for o in range(1, groups):
            z_copies[c * (groups - 1) + o - 1].wait_recv()

        def add(k, carry):
            at = pl.multiple_of(k * width, width)
            total = own[c * part : (c + 1) * part, pl.ds(at, width)].astype(jnp.float32)
            for o in range(1, groups):
                total += got[c][o - 1, :, pl.ds(at, width)].astype(jnp.float32)
            summed[k] = total
            return carry

        lax.fori_loop(0, blocks, add, 0, unroll=4)

        def slot(j, carry):
            total = summed[source[j]] * taken[j]
            ready[c][j] = total
            sq = jnp.sum((total * total).reshape(part // 8, 8, width), axis=0)
            squares[j] = sq if c == 0 else squares[j] + sq
            return carry

        lax.fori_loop(0, slots, slot, 0, unroll=4)

        if c == chunks - 1:
            lane = lax.broadcasted_iota(jnp.int32, (slots, LANES), 1)
            row = lax.broadcasted_iota(jnp.int32, (slots, LANES), 0)
            per_slot = jnp.sum(jnp.sum(squares[...], axis=1), axis=1, keepdims=True)
            shard_part[...] = jnp.sum(jnp.where(lane == row, per_slot, 0.0), axis=0, keepdims=True)
            s_copies = []
            for o in range(1, shards):
                copy = pltpu.make_async_remote_copy(
                    src_ref=shard_part,
                    dst_ref=shard_all.at[o - 1],
                    send_sem=s_send.at[o - 1],
                    recv_sem=s_recv.at[o - 1],
                    device_id=(grp, shard_peer(o)),
                    device_id_type=MESH,
                )
                copy.start()
                s_copies.append(copy)

        for o in range(1, shards):
            copy = pltpu.make_async_remote_copy(
                src_ref=ready[c].at[pl.ds(shard_peer(o) * slots_dev, slots_dev)],
                dst_ref=out_ref.at[:, shard, pl.ds(c * part, part), :],
                send_sem=a_send.at[c, o - 1],
                recv_sem=a_recv.at[c, o - 1],
                device_id=(grp, shard_peer(o)),
                device_id_type=MESH,
            )
            copy.start()
            a_copies.append(copy)
        copy = pltpu.make_async_copy(
            ready[c].at[pl.ds(shard * slots_dev, slots_dev)],
            out_ref.at[:, shard, pl.ds(c * part, part), :],
            keep_sem.at[c],
        )
        copy.start()
        a_copies.append(copy)

    total = shard_part[...]
    for o in range(1, shards):
        s_copies[o - 1].wait()
        total = total + shard_all[o - 1]
    grp_part[...] = total
    g_copies = []
    for o in range(1, groups):
        copy = pltpu.make_async_remote_copy(
            src_ref=grp_part,
            dst_ref=grp_all.at[o - 1],
            send_sem=g_send.at[o - 1],
            recv_sem=g_recv.at[o - 1],
            device_id=(grp_peer(o), shard),
            device_id_type=MESH,
        )
        copy.start()
        g_copies.append(copy)
    lane = lax.broadcasted_iota(jnp.int32, (1, LANES), 1)

    def lay(j, kinds):
        return jnp.where(lane == j, kind_of[j], kinds)

    kinds = lax.fori_loop(0, slots, lay, jnp.full((1, LANES), 3, jnp.int32))
    for o in range(1, groups):
        g_copies[o - 1].wait()
        total = total + grp_all[o - 1]
    root = jnp.sqrt(total / (D * HS))
    for i in range(slots_dev):
        head_ref[i] = jnp.sum(jnp.where(lane == shard * slots_dev + i, root, 0.0))
    for t, heads in enumerate((QH, KVH, KVH)):
        one = jnp.sum(jnp.where(kinds == t, total, 0.0), axis=1, keepdims=True)
        type_ref[t] = jnp.sum(jnp.sqrt(one / (heads * D * HS)))

    for copy in z_copies:
        copy.wait_send()
    for copy in a_copies:
        copy.wait()


def any_step(x, joined, slot, groups, shards, blocks, slots_dev, rows, width):
    slots = slots_dev * shards
    cols = blocks * width
    part = chunk_rows(rows)
    chunks = rows // part
    dma = pltpu.SemaphoreType.DMA
    return pl.pallas_call(
        functools.partial(any_kernel, groups, shards, blocks, slots_dev, chunks),
        out_shape=[
            jax.ShapeDtypeStruct((slots_dev, shards, rows, width), jnp.float32),
            jax.ShapeDtypeStruct((slots_dev,), jnp.float32),
            jax.ShapeDtypeStruct((3,), jnp.float32),
        ],
        in_specs=[
            pl.BlockSpec(memory_space=pltpu.HBM),
            pl.BlockSpec(memory_space=pltpu.SMEM),
            pl.BlockSpec(memory_space=pltpu.SMEM),
        ],
        out_specs=[
            pl.BlockSpec(memory_space=pl.ANY),
            pl.BlockSpec(memory_space=pltpu.SMEM),
            pl.BlockSpec(memory_space=pltpu.SMEM),
        ],
        scratch_shapes=[pltpu.VMEM((rows, cols), jnp.bfloat16)]
        + [pltpu.VMEM((groups - 1, part, cols), jnp.bfloat16)] * chunks
        + [pltpu.VMEM((slots, part, width), jnp.float32)] * chunks
        + [
            pltpu.SMEM((slots,), jnp.int32),
            pltpu.SMEM((slots,), jnp.float32),
            pltpu.SMEM((slots,), jnp.int32),
            pltpu.VMEM((blocks, part, width), jnp.float32),
            pltpu.VMEM((slots, 8, width), jnp.float32),
            pltpu.VMEM((1, LANES), jnp.float32),
            pltpu.VMEM((shards - 1, 1, LANES), jnp.float32),
            pltpu.VMEM((1, LANES), jnp.float32),
            pltpu.VMEM((groups - 1, 1, LANES), jnp.float32),
            dma,
            dma((chunks, groups - 1)),
            dma((chunks, groups - 1)),
            dma((chunks, shards - 1)),
            dma((chunks, shards - 1)),
            dma((chunks,)),
            dma((shards - 1,)),
            dma((shards - 1,)),
            dma((groups - 1,)),
            dma((groups - 1,)),
        ],
        compiler_params=pltpu.CompilerParams(
            collective_id=0,
            has_side_effects=True,
            vmem_limit_bytes=60 * 1024 * 1024,
        ),
    )(x, joined, slot)


def solution(mesh):
    groups, shards = mesh.shape["grp"], mesh.shape["shard"]

    def step(x, joined, slot):
        blocks = joined.shape[0]
        slots_dev = (blocks + shards - 1) // shards
        rows = x.shape[1] // groups
        width = x.shape[2] // blocks
        line = groups == 4 and shards == 8 and rows == 16 * PART and blocks % GROUP == 0
        if line and width == LANES and slots_dev * shards <= LANES:
            return tuple(line_step(x, joined, slot, blocks, slots_dev, shards, rows, width))
        return tuple(any_step(x, joined, slot, groups, shards, blocks, slots_dev, rows, width))

    return jax.shard_map(
        step,
        mesh=mesh,
        in_specs=(P("grp", "shard", None), P(), P()),
        out_specs=(P("shard", None, "grp", None), P("shard"), P()),
        check_vma=False,
    )
```

```python
import functools

import jax
import jax.numpy as jnp
from jax import lax
from jax.experimental import pallas as pl
from jax.experimental.pallas import tpu as pltpu
from jax.sharding import PartitionSpec as P

D = 4096
QH = 32
KVH = 8
HS = 128
LANES = 128
MESH = pl.DeviceIdType.MESH


def chunk_rows(rows):
    return 16 if rows % 16 == 0 else rows


PART = 8
GROUP = 8
QMAX = 524286.0
SMALL = 2.0**-64
LATE = 5
PLAN = (("FNFNLFNLFNFNLFNLFNFNLMA", 1), ("FNFNM", 4), ("M", 6))
HOLD = 4
AHEAD = 4
LAG = 3


def encode(tiles):
    peak = functools.reduce(jnp.maximum, [jnp.abs(t) for t in tiles])
    peak = jnp.max(peak, axis=0, keepdims=True)
    lift = jnp.where(peak < SMALL, 1.0 / SMALL, 1.0)
    scale = QMAX / jnp.maximum(peak * lift, SMALL)
    codes = [jnp.round(t * lift * scale).astype(jnp.int32) for t in tiles]
    half = GROUP // 2
    words = [(codes[i] << 12) | (codes[half + i] & 4095) for i in range(half)]
    tops = [((codes[half + i] >> 12) & 255) << (8 * i) for i in range(half)]
    words.append(functools.reduce(jnp.bitwise_or, tops))
    return words, peak


def decode(words, peak):
    half = GROUP // 2
    codes = [words[i] >> 12 for i in range(half)]
    for i in range(half):
        top = (words[half] << (24 - 8 * i)) >> 24
        codes.append((top << 12) | (words[i] & 4095))
    return [c.astype(jnp.float32) * (1.0 / QMAX) * peak for c in codes]


def flip(s, o):
    for b in range(3):
        if o >> b & 1:
            s = s + (1 - 2 * lax.rem(lax.div(s, 1 << b), 2)) * (1 << b)
    return s


def line_kernel(
    blocks,
    slots_dev,
    x_ref,
    joined_ref,
    slot_ref,
    out_ref,
    total_ref,
    kinds_ref,
    own,
    far,
    passed,
    got,
    out_words,
    out_peaks,
    in_words,
    in_peaks,
    ready,
    late_src,
    late_mine,
    late_in,
    late_raw,
    late_words,
    late_peaks,
    back_words,
    back_peaks,
    source,
    taken,
    kind_of,
    summed,
    squares,
    grp_part,
    grp_all,
    shard_part,
    shard_all,
    own_sem,
    far_sem,
    plane_sem,
    beyond_sem,
    r_send,
    r_recv,
    m_send,
    m_recv,
    w_send,
    w_recv,
    p_send,
    p_recv,
    a_send,
    a_recv,
    keep_sem,
    g_send,
    g_recv,
    s_send,
    s_recv,
    late_sem,
    lx_send,
    lx_recv,
    lk_sem,
    lf_send,
    lf_recv,
    la_send,
    la_recv,
):
    groups, shards = 4, 8
    grp = lax.axis_index("grp")
    shard = lax.axis_index("shard")
    slots = slots_dev * shards
    chunks = own.shape[0]
    width = own.shape[2] // blocks
    sets = blocks // GROUP
    span = GROUP * width

    outer = (grp == 0) | (grp == groups - 1)
    inner = jnp.logical_not(outer)
    mate = grp + 1 - 2 * lax.rem(grp, 2)
    near = jnp.where(outer, 3 - mate, 3 - grp)
    beyond = near + 1 - 2 * lax.rem(near, 2)
    dests = (near, beyond)

    own_copy = pltpu.make_async_copy(x_ref.at[pl.ds(grp * chunks, chunks)], own, own_sem)

    def far_copy(f):
        return pltpu.make_async_copy(
            x_ref.at[pl.ds(dests[f] * chunks, chunks)], far.at[f], far_sem.at[f]
        )

    def send(src, dst, send_sem, recv_sem, to):
        return pltpu.make_async_remote_copy(
            src_ref=src,
            dst_ref=dst,
            send_sem=send_sem,
            recv_sem=recv_sem,
            device_id=to,
            device_id_type=MESH,
        )

    def relay_copy(c, f):
        src = x_ref.at[dests[f] * chunks + c]
        return send(src, passed.at[c, f], r_send.at[c, f], r_recv.at[c, f], (mate, shard))

    def mate_copy(c):
        src = x_ref.at[mate * chunks + c]
        return send(src, got.at[c], m_send.at[c], m_recv.at[c], (mate, shard))

    def coded_copies(c, f):
        to = (dests[f], shard)
        return (
            send(out_words.at[c, f], in_words.at[c], w_send.at[c, f], w_recv.at[c], to),
            send(out_peaks.at[c, f], in_peaks.at[c], p_send.at[c, f], p_recv.at[c], to),
        )

    order = (6, 7, 2, 4, 3, 5, 1)

    def rows_copy(c, o):
        to = flip(shard, o)
        return send(
            ready.at[c, pl.ds(to * slots_dev, slots_dev)],
            out_ref.at[:, shard, pl.ds(pl.multiple_of(c * PART, PART), PART), :],
            a_send.at[c, o - 1],
            a_recv.at[c, o - 1],
            (grp, to),
        )

    def keep_copy(c):
        return pltpu.make_async_copy(
            ready.at[c, pl.ds(shard * slots_dev, slots_dev)],
            out_ref.at[:, shard, pl.ds(pl.multiple_of(c * PART, PART), PART), :],
            keep_sem.at[c],
        )

    def settle(c):
        for o in order:
            rows_copy(c, o).wait()
        keep_copy(c).wait()

    late_copy = pltpu.make_async_copy(x_ref.at[pl.ds(mate * chunks, LATE)], late_src, late_sem)

    def swap_copy(o):
        to = flip(shard, o)
        return send(
            late_mine.at[:, pl.ds(to * slots_dev, slots_dev)],
            late_in.at[shard],
            lx_send.at[o - 1],
            lx_recv.at[o - 1],
            (grp, to),
        )

    stay_copy = pltpu.make_async_copy(
        late_mine.at[:, pl.ds(shard * slots_dev, slots_dev)], late_in.at[shard], lk_sem
    )

    def forward_copy(n):
        to = (mate, shard)
        return send(late_in.at[:, n], late_raw.at[:, n], lf_send.at[n], lf_recv.at[n], to)

    def back_copies():
        to = (mate, shard)
        return (
            send(late_words, back_words, la_send.at[0], la_recv.at[0], to),
            send(late_peaks, back_peaks, la_send.at[1], la_recv.at[1], to),
        )

    own_copy.start()

    barrier = pltpu.get_barrier_semaphore()
    pl.semaphore_signal(barrier, 1, device_id=(mate, shard), device_id_type=MESH)
    for o in range(1, 6):
        pl.semaphore_signal(barrier, 1, device_id=(grp, flip(shard, o)), device_id_type=MESH)

    @pl.when(inner)
    def _():
        pl.semaphore_signal(barrier, 1, device_id=(near, shard), device_id_type=MESH)
        pl.semaphore_wait(barrier, 7)
        pl.semaphore_signal(beyond_sem, 1, device_id=(near, shard), device_id_type=MESH)
        for f in range(2):
            far_copy(f).start()
        for c in range(AHEAD):
            mate_copy(c).start()

    @pl.when(outer)
    def _():
        pl.semaphore_wait(barrier, 6)
        done = dict(N=0, F=0, M=LATE)
        for pattern, times in PLAN:
            now, per = dict(done), {k: pattern.count(k) for k in done}

            def queue(k, carry, pattern=pattern, now=now, per=per):
                at = {key: now[key] + k * per[key] for key in now}
                for kind in pattern:
                    if kind in "NF":
                        relay_copy(at[kind], "NF".index(kind)).start()
                    elif kind == "M":
                        mate_copy(at[kind]).start()
                    if kind in at:
                        at[kind] += 1
                return carry

            lax.fori_loop(0, times, queue, 0)
            done = {key: now[key] + times * per[key] for key in now}
        late_copy.start()

    pl.semaphore_signal(plane_sem, 1, device_id=(grp, flip(shard, 2)), device_id_type=MESH)

    def find(j, carry):
        head = jnp.int32(-1)
        for b in range(blocks):
            head = jnp.where(slot_ref[b] == j, b, head)
        there = head >= 0
        source[j] = jnp.where(there, joined_ref[jnp.maximum(head, 0)], 0)
        taken[j] = jnp.where(there, 1.0, 0.0)
        kind = jnp.where(head >= QH, 1, 0) + jnp.where(head >= QH + KVH, 1, 0)
        kind_of[j] = jnp.where(there, kind, 3)
        return carry

    lax.fori_loop(0, slots, find, 0)
    own_copy.wait()

    def clear(j, carry):
        squares[j] = jnp.zeros((PART, width), jnp.float32)
        return carry

    lax.fori_loop(0, slots, clear, 0)

    def pack(c, f):
        relay_copy(c, f).wait_recv()

        def pack_set(p, carry):
            at = pl.ds(pl.multiple_of(p * span, span), span)
            total = far[f, c, :, at].astype(jnp.float32) + passed[c, f, :, at].astype(jnp.float32)
            words, peak = encode([total[:, i * width : (i + 1) * width] for i in range(GROUP)])
            for i, word in enumerate(words):
                out_words[c, f, p, i] = word
            out_peaks[c, f, p] = peak
            return carry

        lax.fori_loop(0, sets, pack_set, 0, unroll=2)
        for copy in coded_copies(c, f):
            copy.start()
        if f == 1:

            @pl.when(c + AHEAD < chunks)
            def _():
                mate_copy(c + AHEAD).start()

    def finish(c, late=False):
        for copy in coded_copies(c, 0):
            copy.wait_recv()

        def pre_set(p, carry):
            at = pl.ds(pl.multiple_of(p * span, span), span)
            mine = own[c, :, at].astype(jnp.float32)
            tiles = decode([in_words[c, p, i] for i in range(GROUP // 2 + 1)], in_peaks[c, p])
            for i, tile in enumerate(tiles):
                summed[p * GROUP + i] = mine[:, i * width : (i + 1) * width] + tile
            return carry

        lax.fori_loop(0, sets, pre_set, 0, unroll=2)
        if not late:
            mate_copy(c).wait_recv()

        def add_set(p, carry):
            at = pl.ds(pl.multiple_of(p * span, span), span)
            more = got[c, :, at].astype(jnp.float32)
            for i in range(GROUP):
                summed[p * GROUP + i] += more[:, i * width : (i + 1) * width]
            return carry

        if not late:
            lax.fori_loop(0, sets, add_set, 0, unroll=2)

        def place(j, carry):
            total = summed[source[j]] * taken[j]
            ready[c, j] = total
            if not late:
                squares[j] += total * total
            return carry

        lax.fori_loop(0, slots, place, 0, unroll=8)
        for o in order:
            rows_copy(c, o).start()
        keep_copy(c).start()

    def tell(j, carry):
        for n in range(LATE):
            at = pl.ds(n * PART, PART)
            words, peak = encode([out_ref[j, a, at, :] for a in range(shards)])
            for i, word in enumerate(words):
                late_words[n, j, i] = word
            late_peaks[n, j] = peak
        return carry

    def finish_and_settle(c, carry=0, first=0):
        finish(c)

        @pl.when(c >= first + LAG)
        def _():
            settle(c - LAG)

        return carry

    @pl.when(inner)
    def _():
        for f in range(2):
            far_copy(f).wait()
        pl.semaphore_wait(beyond_sem, 1)
        pl.semaphore_wait(plane_sem, 1)
        done = dict(N=0, F=0, L=0, M=LATE)
        for pattern, times in PLAN:
            now, per = dict(done), {k: pattern.count(k) for k in done}

            def act(k, carry, pattern=pattern, now=now, per=per):
                at = {key: now[key] + k * per[key] for key in now}
                for kind in pattern:
                    if kind in "NF":
                        pack(at[kind], "NF".index(kind))
                    elif kind == "M":
                        finish_and_settle(at[kind], first=LATE)
                    elif kind == "L":
                        finish(at[kind], late=True)
                    else:
                        for c in range(LATE):
                            settle(c)
                        lax.fori_loop(0, slots_dev, tell, 0)
                        for copy in back_copies():
                            copy.start()
                    if kind in at:
                        at[kind] += 1
                return carry

            lax.fori_loop(0, times, act, 0)
            done = {key: now[key] + times * per[key] for key in now}

    @pl.when(outer)
    def _():
        pl.semaphore_wait(plane_sem, 1)
        late_copy.wait()

        for n in range(LATE):

            def split(p, carry, n=n):
                at = pl.ds(pl.multiple_of(p * span, span), span)
                rows = late_src[n, :, at].astype(jnp.float32)
                for i in range(GROUP):
                    summed[p * GROUP + i] = rows[:, i * width : (i + 1) * width]
                return carry

            lax.fori_loop(0, sets, split, 0, unroll=2)

            def arrange(j, carry, n=n):
                late_mine[n, j] = (summed[source[j]] * taken[j]).astype(jnp.bfloat16)
                return carry

            lax.fori_loop(0, slots, arrange, 0, unroll=4)
        for o in order:
            swap_copy(o).start()
        stay_copy.start()
        for o in order:
            swap_copy(o).wait()
        stay_copy.wait()
        for n in range(LATE - HOLD):
            forward_copy(n).start()
        lax.fori_loop(0, chunks - LAG, finish_and_settle, 0)
        for copy in back_copies():
            copy.wait_recv()

        def late_squares(j, carry):
            acc = jnp.zeros((PART, width), jnp.float32)
            for n in range(LATE):
                tiles = decode([back_words[n, j, i] for i in range(GROUP // 2 + 1)], back_peaks[n, j])
                for a, tile in enumerate(tiles):
                    total = tile + late_in[a, n, j].astype(jnp.float32)
                    acc += total * total
            squares[shard * slots_dev + j] += acc
            return carry

        lax.fori_loop(0, slots_dev, late_squares, 0)
        lax.fori_loop(chunks - LAG, chunks, finish_and_settle, 0)

    lane = lax.broadcasted_iota(jnp.int32, (slots, LANES), 1)
    row = lax.broadcasted_iota(jnp.int32, (slots, LANES), 0)
    per_slot = jnp.sum(jnp.sum(squares[...], axis=1), axis=1, keepdims=True)
    total = jnp.sum(jnp.where(lane == row, per_slot, 0.0), axis=0, keepdims=True)

    def grp_copy(o):
        to = lax.rem(grp + o, groups)
        return send(grp_part, grp_all.at[o - 1], g_send.at[o - 1], g_recv.at[o - 1], (to, shard))

    def shard_copy(o):
        to = flip(shard, o)
        return send(
            shard_part, shard_all.at[o - 1], s_send.at[o - 1], s_recv.at[o - 1], (grp, to)
        )

    grp_part[...] = total
    for o in range(1, groups):
        grp_copy(o).start()

    @pl.when(outer)
    def _():
        for n in range(LATE - HOLD, LATE):
            forward_copy(n).start()

    lane = lax.broadcasted_iota(jnp.int32, (1, LANES), 1)

    def lay(j, kinds):
        return jnp.where(lane == j, kind_of[j], kinds)

    kinds = lax.fori_loop(0, slots, lay, jnp.full((1, LANES), 3, jnp.int32))

    @pl.when(inner)
    def _():
        def drain(c, carry):
            mate_copy(c).wait_send()
            for f in range(2):
                for copy in coded_copies(c, f):
                    copy.wait_send()
            return carry

        lax.fori_loop(0, chunks, drain, 0)
        for copy in back_copies():
            copy.wait_send()

    @pl.when(outer)
    def _():
        def drain(c, carry):
            for f in range(2):
                relay_copy(c, f).wait_send()

            @pl.when(c >= LATE)
            def _():
                mate_copy(c).wait_send()

            return carry

        lax.fori_loop(0, chunks, drain, 0)

    for o in range(1, groups):
        grp_copy(o).wait()
        total = total + grp_all[o - 1]
    shard_part[...] = total
    for o in order:
        shard_copy(o).start()
    for c in range(chunks - LAG, chunks):
        settle(c)
    for o in order:
        shard_copy(o).wait()
        total = total + shard_all[o - 1]
    total_ref[...] = total
    kinds_ref[...] = kinds

    @pl.when(outer)
    def _():
        for n in range(LATE):
            forward_copy(n).wait_send()

    @pl.when(inner)
    def _():
        for n in range(LATE):
            forward_copy(n).wait_recv()

            def add_late(a, carry, n=n):
                for j in range(slots_dev):
                    at = pl.ds(n * PART, PART)
                    out_ref[j, a, at, :] += late_raw[a, n, j].astype(jnp.float32)
                return carry

            lax.fori_loop(0, shards, add_late, 0, unroll=True)


def store_kernel(slots_dev, in_ref, total_ref, kinds_ref, out_ref, head_ref, type_ref, heads, types, sems):
    copies = [
        pltpu.make_async_copy(in_ref.at[j], out_ref.at[j], sems.at[j]) for j in range(slots_dev)
    ]
    copies.append(pltpu.make_async_copy(heads, head_ref, sems.at[slots_dev]))
    copies.append(pltpu.make_async_copy(types, type_ref, sems.at[slots_dev + 1]))
    for copy in copies[:slots_dev]:
        copy.start()
    shard = lax.axis_index("shard")
    total = total_ref[...]
    kinds = kinds_ref[...]
    lane = lax.broadcasted_iota(jnp.int32, (1, LANES), 1)
    root = jnp.sqrt(total / (D * HS))
    for i in range(slots_dev):
        heads[i] = jnp.sum(jnp.where(lane == shard * slots_dev + i, root, 0.0))
    for t, count in enumerate((QH, KVH, KVH)):
        one = jnp.sum(jnp.where(kinds == t, total, 0.0), axis=1, keepdims=True)
        types[t] = jnp.sum(jnp.sqrt(one / (count * D * HS)))
    for copy in copies[slots_dev:]:
        copy.start()
    for copy in copies:
        copy.wait()


def line_step(x, joined, slot, blocks, slots_dev, shards, rows, width):
    chunks = rows // PART
    cols = blocks * width
    sets = blocks // GROUP
    slots = slots_dev * shards
    half = GROUP // 2
    dma = pltpu.SemaphoreType.DMA
    regular = pltpu.SemaphoreType.REGULAR
    f32, i32, bf16 = jnp.float32, jnp.int32, jnp.bfloat16
    out, total, kinds = pl.pallas_call(
        functools.partial(line_kernel, blocks, slots_dev),
        out_shape=[
            pltpu.VMEM((slots_dev, shards, rows, width), f32),
            pltpu.VMEM((1, LANES), f32),
            pltpu.VMEM((1, LANES), i32),
        ],
        in_specs=[
            pl.BlockSpec(memory_space=pltpu.HBM),
            pl.BlockSpec(memory_space=pltpu.SMEM),
            pl.BlockSpec(memory_space=pltpu.SMEM),
        ],
        out_specs=[pl.BlockSpec(memory_space=pltpu.VMEM)] * 3,
        scratch_shapes=[
            pltpu.VMEM((chunks, PART, cols), bf16),
            pltpu.VMEM((2, chunks, PART, cols), bf16),
            pltpu.VMEM((chunks, 2, PART, cols), bf16),
            pltpu.VMEM((chunks, PART, cols), bf16),
            pltpu.VMEM((chunks, 2, sets, half + 1, PART, width), i32),
            pltpu.VMEM((chunks, 2, sets, 1, width), f32),
            pltpu.VMEM((chunks, sets, half + 1, PART, width), i32),
            pltpu.VMEM((chunks, sets, 1, width), f32),
            pltpu.VMEM((chunks, slots, PART, width), f32),
            pltpu.VMEM((LATE, PART, cols), bf16),
            pltpu.VMEM((LATE, slots, PART, width), bf16),
            pltpu.VMEM((shards, LATE, slots_dev, PART, width), bf16),
            pltpu.VMEM((shards, LATE, slots_dev, PART, width), bf16),
            pltpu.VMEM((LATE, slots_dev, half + 1, PART, width), i32),
            pltpu.VMEM((LATE, slots_dev, 1, width), f32),
            pltpu.VMEM((LATE, slots_dev, half + 1, PART, width), i32),
            pltpu.VMEM((LATE, slots_dev, 1, width), f32),
            pltpu.SMEM((slots,), i32),
            pltpu.SMEM((slots,), f32),
            pltpu.SMEM((slots,), i32),
            pltpu.VMEM((blocks, PART, width), f32),
            pltpu.VMEM((slots, PART, width), f32),
            pltpu.VMEM((1, LANES), f32),
            pltpu.VMEM((3, 1, LANES), f32),
            pltpu.VMEM((1, LANES), f32),
            pltpu.VMEM((shards - 1, 1, LANES), f32),
            dma,
            dma((2,)),
            regular,
            regular,
            dma((chunks, 2)),
            dma((chunks, 2)),
            dma((chunks,)),
            dma((chunks,)),
            dma((chunks, 2)),
            dma((chunks,)),
            dma((chunks, 2)),
            dma((chunks,)),
            dma((chunks, shards - 1)),
            dma((chunks, shards - 1)),
            dma((chunks,)),
            dma((3,)),
            dma((3,)),
            dma((shards - 1,)),
            dma((shards - 1,)),
            dma,
            dma((shards - 1,)),
            dma((shards - 1,)),
            dma,
            dma((LATE,)),
            dma((LATE,)),
            dma((2,)),
            dma((2,)),
        ],
        compiler_params=pltpu.CompilerParams(
            collective_id=0,
            has_side_effects=True,
            vmem_limit_bytes=57 * 1024 * 1024,
        ),
    )(x.reshape(4 * chunks, PART, cols), joined, slot)
    return pl.pallas_call(
        functools.partial(store_kernel, slots_dev),
        out_shape=[
            jax.ShapeDtypeStruct((slots_dev, shards, rows, width), f32),
            jax.ShapeDtypeStruct((slots_dev,), f32),
            jax.ShapeDtypeStruct((3,), f32),
        ],
        in_specs=[pl.BlockSpec(memory_space=pltpu.VMEM)] * 3,
        out_specs=[pl.BlockSpec(memory_space=pltpu.HBM)] * 3,
        scratch_shapes=[
            pltpu.SMEM((slots_dev,), f32),
            pltpu.SMEM((3,), f32),
            dma((slots_dev + 2,)),
        ],
        compiler_params=pltpu.CompilerParams(vmem_limit_bytes=1024 * 1024),
    )(out, total, kinds)


def any_kernel(groups, shards, blocks, slots_dev, chunks, *refs):
    x_ref, joined_ref, slot_ref = refs[:3]
    out_ref, head_ref, type_ref = refs[3:6]
    own = refs[6]
    got = refs[7 : 7 + chunks]
    ready = refs[7 + chunks : 7 + 2 * chunks]
    rest = refs[7 + 2 * chunks :]
    (source, taken, kind_of, summed, squares, shard_part, shard_all, grp_part, grp_all) = rest[:9]
    (own_sem, z_send, z_recv, a_send, a_recv, keep_sem, s_send, s_recv, g_send, g_recv) = rest[9:]

    grp = lax.axis_index("grp")
    shard = lax.axis_index("shard")
    slots = slots_dev * shards
    rows = own.shape[0]
    part = rows // chunks
    width = own.shape[1] // blocks

    def grp_peer(offset):
        return lax.rem(grp + offset, groups)

    def shard_peer(offset):
        return lax.rem(shard + offset, shards)

    load_own = pltpu.make_async_copy(
        x_ref.at[0, pl.ds(pl.multiple_of(grp * rows, 8), rows), :], own, own_sem
    )
    load_own.start()

    barrier = pltpu.get_barrier_semaphore()
    for o in range(1, groups):
        pl.semaphore_signal(barrier, 1, device_id=(grp_peer(o), shard), device_id_type=MESH)
    for o in range(1, shards):
        pl.semaphore_signal(barrier, 1, device_id=(grp, shard_peer(o)), device_id_type=MESH)
    pl.semaphore_wait(barrier, groups + shards - 2)

    z_copies = []
    for c in range(chunks):
        for o in range(1, groups):
            first = pl.multiple_of(grp_peer(o) * rows + c * part, 8)
            copy = pltpu.make_async_remote_copy(
                src_ref=x_ref.at[0, pl.ds(first, part), :],
                dst_ref=got[c].at[o - 1],
                send_sem=z_send.at[c, o - 1],
                recv_sem=z_recv.at[c, o - 1],
                device_id=(grp_peer(o), shard),
                device_id_type=MESH,
            )
            copy.start()
            z_copies.append(copy)

    def find(j, carry):
        found, block, kind = jnp.float32(0), jnp.int32(0), jnp.int32(3)
        for b in range(blocks):
            hit = slot_ref[b] == j
            found = jnp.where(hit, 1.0, found)
            block = jnp.where(hit, joined_ref[b], block)
            kind = jnp.where(hit, (b >= QH) + (b >= QH + KVH), kind)
        source[j] = block
        taken[j] = found
        kind_of[j] = kind
        return carry

    lax.fori_loop(0, slots, find, 0)

    load_own.wait()
    a_copies = []
    for c in range(chunks):
        for o in range(1, groups):
            z_copies[c * (groups - 1) + o - 1].wait_recv()

        def add(k, carry):
            at = pl.multiple_of(k * width, width)
            total = own[c * part : (c + 1) * part, pl.ds(at, width)].astype(jnp.float32)
            for o in range(1, groups):
                total += got[c][o - 1, :, pl.ds(at, width)].astype(jnp.float32)
            summed[k] = total
            return carry

        lax.fori_loop(0, blocks, add, 0, unroll=4)

        def slot(j, carry):
            total = summed[source[j]] * taken[j]
            ready[c][j] = total
            sq = jnp.sum((total * total).reshape(part // 8, 8, width), axis=0)
            squares[j] = sq if c == 0 else squares[j] + sq
            return carry

        lax.fori_loop(0, slots, slot, 0, unroll=4)

        if c == chunks - 1:
            lane = lax.broadcasted_iota(jnp.int32, (slots, LANES), 1)
            row = lax.broadcasted_iota(jnp.int32, (slots, LANES), 0)
            per_slot = jnp.sum(jnp.sum(squares[...], axis=1), axis=1, keepdims=True)
            shard_part[...] = jnp.sum(jnp.where(lane == row, per_slot, 0.0), axis=0, keepdims=True)
            s_copies = []
            for o in range(1, shards):
                copy = pltpu.make_async_remote_copy(
                    src_ref=shard_part,
                    dst_ref=shard_all.at[o - 1],
                    send_sem=s_send.at[o - 1],
                    recv_sem=s_recv.at[o - 1],
                    device_id=(grp, shard_peer(o)),
                    device_id_type=MESH,
                )
                copy.start()
                s_copies.append(copy)

        for o in range(1, shards):
            copy = pltpu.make_async_remote_copy(
                src_ref=ready[c].at[pl.ds(shard_peer(o) * slots_dev, slots_dev)],
                dst_ref=out_ref.at[:, shard, pl.ds(c * part, part), :],
                send_sem=a_send.at[c, o - 1],
                recv_sem=a_recv.at[c, o - 1],
                device_id=(grp, shard_peer(o)),
                device_id_type=MESH,
            )
            copy.start()
            a_copies.append(copy)
        copy = pltpu.make_async_copy(
            ready[c].at[pl.ds(shard * slots_dev, slots_dev)],
            out_ref.at[:, shard, pl.ds(c * part, part), :],
            keep_sem.at[c],
        )
        copy.start()
        a_copies.append(copy)

    total = shard_part[...]
    for o in range(1, shards):
        s_copies[o - 1].wait()
        total = total + shard_all[o - 1]
    grp_part[...] = total
    g_copies = []
    for o in range(1, groups):
        copy = pltpu.make_async_remote_copy(
            src_ref=grp_part,
            dst_ref=grp_all.at[o - 1],
            send_sem=g_send.at[o - 1],
            recv_sem=g_recv.at[o - 1],
            device_id=(grp_peer(o), shard),
            device_id_type=MESH,
        )
        copy.start()
        g_copies.append(copy)
    lane = lax.broadcasted_iota(jnp.int32, (1, LANES), 1)

    def lay(j, kinds):
        return jnp.where(lane == j, kind_of[j], kinds)

    kinds = lax.fori_loop(0, slots, lay, jnp.full((1, LANES), 3, jnp.int32))
    for o in range(1, groups):
        g_copies[o - 1].wait()
        total = total + grp_all[o - 1]
    root = jnp.sqrt(total / (D * HS))
    for i in range(slots_dev):
        head_ref[i] = jnp.sum(jnp.where(lane == shard * slots_dev + i, root, 0.0))
    for t, heads in enumerate((QH, KVH, KVH)):
        one = jnp.sum(jnp.where(kinds == t, total, 0.0), axis=1, keepdims=True)
        type_ref[t] = jnp.sum(jnp.sqrt(one / (heads * D * HS)))

    for copy in z_copies:
        copy.wait_send()
    for copy in a_copies:
        copy.wait()


def any_step(x, joined, slot, groups, shards, blocks, slots_dev, rows, width):
    slots = slots_dev * shards
    cols = blocks * width
    part = chunk_rows(rows)
    chunks = rows // part
    dma = pltpu.SemaphoreType.DMA
    return pl.pallas_call(
        functools.partial(any_kernel, groups, shards, blocks, slots_dev, chunks),
        out_shape=[
            jax.ShapeDtypeStruct((slots_dev, shards, rows, width), jnp.float32),
            jax.ShapeDtypeStruct((slots_dev,), jnp.float32),
            jax.ShapeDtypeStruct((3,), jnp.float32),
        ],
        in_specs=[
            pl.BlockSpec(memory_space=pltpu.HBM),
            pl.BlockSpec(memory_space=pltpu.SMEM),
            pl.BlockSpec(memory_space=pltpu.SMEM),
        ],
        out_specs=[
            pl.BlockSpec(memory_space=pl.ANY),
            pl.BlockSpec(memory_space=pltpu.SMEM),
            pl.BlockSpec(memory_space=pltpu.SMEM),
        ],
        scratch_shapes=[pltpu.VMEM((rows, cols), jnp.bfloat16)]
        + [pltpu.VMEM((groups - 1, part, cols), jnp.bfloat16)] * chunks
        + [pltpu.VMEM((slots, part, width), jnp.float32)] * chunks
        + [
            pltpu.SMEM((slots,), jnp.int32),
            pltpu.SMEM((slots,), jnp.float32),
            pltpu.SMEM((slots,), jnp.int32),
            pltpu.VMEM((blocks, part, width), jnp.float32),
            pltpu.VMEM((slots, 8, width), jnp.float32),
            pltpu.VMEM((1, LANES), jnp.float32),
            pltpu.VMEM((shards - 1, 1, LANES), jnp.float32),
            pltpu.VMEM((1, LANES), jnp.float32),
            pltpu.VMEM((groups - 1, 1, LANES), jnp.float32),
            dma,
            dma((chunks, groups - 1)),
            dma((chunks, groups - 1)),
            dma((chunks, shards - 1)),
            dma((chunks, shards - 1)),
            dma((chunks,)),
            dma((shards - 1,)),
            dma((shards - 1,)),
            dma((groups - 1,)),
            dma((groups - 1,)),
        ],
        compiler_params=pltpu.CompilerParams(
            collective_id=0,
            has_side_effects=True,
            vmem_limit_bytes=60 * 1024 * 1024,
        ),
    )(x, joined, slot)


def solution(mesh):
    groups, shards = mesh.shape["grp"], mesh.shape["shard"]

    def step(x, joined, slot):
        blocks = joined.shape[0]
        slots_dev = (blocks + shards - 1) // shards
        rows = x.shape[1] // groups
        width = x.shape[2] // blocks
        line = groups == 4 and shards == 8 and rows == 16 * PART and blocks % GROUP == 0
        if line and width == LANES and slots_dev * shards <= LANES:
            return tuple(line_step(x, joined, slot, blocks, slots_dev, shards, rows, width))
        return tuple(any_step(x, joined, slot, groups, shards, blocks, slots_dev, rows, width))

    return jax.shard_map(
        step,
        mesh=mesh,
        in_specs=(P("grp", "shard", None), P(), P()),
        out_specs=(P("shard", None, "grp", None), P("shard"), P()),
        check_vma=False,
    )
```

```python
import functools

import jax
import jax.numpy as jnp
from jax import lax
from jax.experimental import pallas as pl
from jax.experimental.pallas import tpu as pltpu
from jax.sharding import PartitionSpec as P

D = 4096
QH = 32
KVH = 8
HS = 128
LANES = 128
MESH = pl.DeviceIdType.MESH


def chunk_rows(rows):
    return 16 if rows % 16 == 0 else rows


PART = 8
GROUP = 8
QMAX = 524286.0
SMALL = 2.0**-64
LATE = 5
LATE_COPIES = ((0, 1), (1, 2), (3, 2))
SINGLE = 2
PLAN = (("FNFNLfnLflnfnLMfAnm", 1), ("fnm", 3), ("m", 1))
AHEAD = 4


def pieces(first, last):
    c, found = first, []
    while c < last:
        n = 2 if c % 2 == 0 and c + 2 <= last and c >= SINGLE else 1
        found.append((c, n))
        c += n
    return found


def encode(tiles):
    peak = functools.reduce(jnp.maximum, [jnp.abs(t) for t in tiles])
    peak = jnp.max(peak, axis=0, keepdims=True)
    lift = jnp.where(peak < SMALL, 1.0 / SMALL, 1.0)
    scale = QMAX / jnp.maximum(peak * lift, SMALL)
    codes = [jnp.round(t * lift * scale).astype(jnp.int32) for t in tiles]
    half = GROUP // 2
    words = [(codes[i] << 12) | (codes[half + i] & 4095) for i in range(half)]
    tops = [((codes[half + i] >> 12) & 255) << (8 * i) for i in range(half)]
    words.append(functools.reduce(jnp.bitwise_or, tops))
    return words, peak


def decode(words, peak):
    half = GROUP // 2
    codes = [words[i] >> 12 for i in range(half)]
    for i in range(half):
        top = (words[half] << (24 - 8 * i)) >> 24
        codes.append((top << 12) | (words[i] & 4095))
    return [c.astype(jnp.float32) * (1.0 / QMAX) * peak for c in codes]


def piece(c, n):
    return c if n == 1 else lax.div(c, 2) + SINGLE // 2


def wait_for(ref, sem):
    pltpu.make_async_copy(ref, ref, sem).wait()


def steps(pattern, done):
    per = {k: sum(1 + c.islower() for c in pattern if c.lower() == k) for k in done}
    return dict(done), per


def flip(s, o):
    for b in range(3):
        if o >> b & 1:
            s = s + (1 - 2 * lax.rem(lax.div(s, 1 << b), 2)) * (1 << b)
    return s


def line_kernel(
    blocks,
    slots_dev,
    x_ref,
    joined_hbm,
    slot_hbm,
    out_ref,
    late_raw,
    total_ref,
    kinds_ref,
    joined_ref,
    slot_ref,
    first,
    own,
    far,
    passed,
    got,
    out_words,
    out_peaks,
    in_words,
    in_peaks,
    ready,
    late_src,
    late_mine,
    late_in,
    late_words,
    late_peaks,
    back_words,
    back_peaks,
    source,
    taken,
    kind_of,
    summed,
    squares,
    grp_part,
    grp_all,
    shard_part,
    shard_all,
    index_sem,
    first_sem,
    own_sem,
    far_sem,
    plane_sem,
    beyond_sem,
    r_send,
    r_recv,
    m_send,
    m_recv,
    w_send,
    w_recv,
    p_send,
    p_recv,
    a_send,
    a_recv,
    a_late,
    g_send,
    g_recv,
    s_send,
    s_recv,
    late_sem,
    lx_send,
    lx_recv,
    lk_sem,
    lf_send,
    lf_recv,
    la_send,
    la_recv,
):
    groups, shards = 4, 8
    grp = lax.axis_index("grp")
    shard = lax.axis_index("shard")
    slots = slots_dev * shards
    chunks = own.shape[0]
    width = own.shape[2] // blocks
    sets = blocks // GROUP
    span = GROUP * width

    outer = (grp == 0) | (grp == groups - 1)
    inner = jnp.logical_not(outer)
    mate = grp + 1 - 2 * lax.rem(grp, 2)
    near = jnp.where(outer, 3 - mate, 3 - grp)
    beyond = near + 1 - 2 * lax.rem(near, 2)
    dests = (near, beyond)

    own_copy = pltpu.make_async_copy(x_ref.at[pl.ds(grp * chunks, chunks)], own, own_sem)

    def far_copy(f):
        return pltpu.make_async_copy(
            x_ref.at[pl.ds(dests[f] * chunks, chunks)], far.at[f], far_sem.at[f]
        )

    def send(src, dst, send_sem, recv_sem, to):
        return pltpu.make_async_remote_copy(
            src_ref=src,
            dst_ref=dst,
            send_sem=send_sem,
            recv_sem=recv_sem,
            device_id=to,
            device_id_type=MESH,
        )

    index_copies = [
        pltpu.make_async_copy(joined_hbm, joined_ref, index_sem.at[0]),
        pltpu.make_async_copy(slot_hbm, slot_ref, index_sem.at[1]),
    ]
    first_copy = pltpu.make_async_copy(x_ref.at[pl.ds(beyond * chunks, 1)], first, first_sem)

    def relay_copy(c, n, f):
        staged = isinstance(c, int) and c == 0 and f == 1
        src = first if staged else x_ref.at[pl.ds(dests[f] * chunks + c, n)]
        dst = passed.at[f, pl.ds(c, n)]
        return send(src, dst, r_send, r_recv.at[piece(c, n), f], (mate, shard))

    def mate_copy(c, n):
        src = x_ref.at[pl.ds(mate * chunks + c, n)]
        return send(src, got.at[pl.ds(c, n)], m_send, m_recv.at[lax.div(c, 2)], (mate, shard))

    def coded_copies(c, n, f):
        to = (dests[f], shard)
        at = pl.ds(c, n)
        return (
            send(out_words.at[f, at], in_words.at[at], w_send, w_recv.at[piece(c, n)], to),
            send(out_peaks.at[f, at], in_peaks.at[at], p_send, p_recv.at[piece(c, n)], to),
        )

    order = (6, 7, 2, 4, 3, 5, 1)

    def rows_of(c, n):
        return pl.ds(pl.multiple_of(c * PART, PART), n * PART)

    def rows_copy(c, n, o, recv_sem):
        to = flip(shard, o)
        return send(
            ready.at[pl.ds(to * slots_dev, slots_dev), rows_of(c, n)],
            out_ref.at[:, shard, rows_of(c, n), :],
            a_send,
            recv_sem,
            (grp, to),
        )

    def others(first, last):
        at = pl.ds(first * PART, (last - first) * PART)
        return ready.at[pl.ds(0, (shards - 1) * slots_dev), at]

    late_copy = pltpu.make_async_copy(x_ref.at[pl.ds(mate * chunks, LATE)], late_src, late_sem)

    def swap_copy(o):
        to = flip(shard, o)
        return send(
            late_mine.at[:, pl.ds(to * slots_dev, slots_dev)],
            late_in.at[shard],
            lx_send,
            lx_recv,
            (grp, to),
        )

    stay_copy = pltpu.make_async_copy(
        late_mine.at[:, pl.ds(shard * slots_dev, slots_dev)], late_in.at[shard], lk_sem
    )

    def forward_copy(i):
        at = pl.ds(*LATE_COPIES[i])
        to = (mate, shard)
        return send(late_in.at[:, at], late_raw.at[:, at], lf_send, lf_recv, to)

    def back_copies():
        to = (mate, shard)
        return (
            send(late_words, back_words, la_send.at[0], la_recv.at[0], to),
            send(late_peaks, back_peaks, la_send.at[1], la_recv.at[1], to),
        )

    first_copy.start()

    barrier = pltpu.get_barrier_semaphore()
    pl.semaphore_signal(barrier, 1, device_id=(mate, shard), device_id_type=MESH)
    for o in range(1, 6):
        pl.semaphore_signal(barrier, 1, device_id=(grp, flip(shard, o)), device_id_type=MESH)

    @pl.when(inner)
    def _():
        pl.semaphore_signal(barrier, 1, device_id=(near, shard), device_id_type=MESH)
        pl.semaphore_wait(barrier, 7)
        own_copy.start()
        pl.semaphore_signal(beyond_sem, 1, device_id=(near, shard), device_id_type=MESH)
        for f in range(2):
            far_copy(f).start()
        for c in range(0, AHEAD, 2):
            mate_copy(c, 2).start()

    @pl.when(outer)
    def _():
        pl.semaphore_wait(barrier, 6)
        first_copy.wait()
        done = dict(n=0, f=0, m=LATE)
        for pattern, times in PLAN:
            now, per = steps(pattern, done)

            def queue(k, carry, pattern=pattern, now=now, per=per):
                at = {key: now[key] + k * per[key] for key in now}
                for kind in pattern:
                    n, key = 1 + kind.islower(), kind.lower()
                    if key in "nf":
                        relay_copy(at[key], n, "nf".index(key)).start()
                    elif key == "m":
                        mate_copy(at[key], n).start()
                    if key in at:
                        at[key] += n
                return carry

            if times == 1:
                queue(0, 0)
            else:
                lax.fori_loop(0, times, queue, 0)
            done = {key: now[key] + times * per[key] for key in now}
        own_copy.start()
        late_copy.start()

    pl.semaphore_signal(plane_sem, 1, device_id=(grp, flip(shard, 2)), device_id_type=MESH)

    def find(j, carry):
        head = jnp.int32(-1)
        for b in range(blocks):
            head = jnp.where(slot_ref[b] == j, b, head)
        there = head >= 0
        source[j] = jnp.where(there, joined_ref[jnp.maximum(head, 0)], 0)
        taken[j] = jnp.where(there, 1.0, 0.0)
        kind = jnp.where(head >= QH, 1, 0) + jnp.where(head >= QH + KVH, 1, 0)
        kind_of[j] = jnp.where(there, kind, 3)
        return carry

    for copy in index_copies:
        copy.start()
    for copy in index_copies:
        copy.wait()
    lax.fori_loop(0, slots, find, 0)
    own_copy.wait()

    def clear(j, carry):
        squares[j] = jnp.zeros((PART, width), jnp.float32)
        return carry

    lax.fori_loop(0, slots, clear, 0)

    def pack(c, n, f):
        relay_copy(c, n, f).wait_recv()

        def pack_set(q, carry):
            i, p = lax.div(q, sets), lax.rem(q, sets)
            at = pl.ds(pl.multiple_of(p * span, span), span)
            total = far[f, c + i, :, at].astype(jnp.float32)
            total += passed[f, c + i, :, at].astype(jnp.float32)
            words, peak = encode([total[:, i * width : (i + 1) * width] for i in range(GROUP)])
            for w, word in enumerate(words):
                out_words[f, c + i, p, w] = word
            out_peaks[f, c + i, p] = peak
            return carry

        lax.fori_loop(0, n * sets, pack_set, 0, unroll=2)
        for copy in coded_copies(c, n, f):
            copy.start()
        if f == 1 and n == 2:

            @pl.when(c + AHEAD - SINGLE < chunks)
            def _():
                mate_copy(c + AHEAD - SINGLE, 2).start()

    def wait_coded(c, n):
        for copy in coded_copies(c, n, 0):
            copy.wait_recv()

    def finish(c, n, arrive):
        for i in range(n):

            def pre_set(p, carry, i=i):
                at = pl.ds(pl.multiple_of(p * span, span), span)
                mine = own[c + i, :, at].astype(jnp.float32)
                words = [in_words[c + i, p, w] for w in range(GROUP // 2 + 1)]
                for t, tile in enumerate(decode(words, in_peaks[c + i, p])):
                    summed[i, p * GROUP + t] = mine[:, t * width : (t + 1) * width] + tile
                return carry

            lax.fori_loop(0, sets, pre_set, 0, unroll=2)
        if arrive is not None:
            arrive()
        for i in range(n):

            def add_set(p, carry, i=i):
                at = pl.ds(pl.multiple_of(p * span, span), span)
                more = got[c + i, :, at].astype(jnp.float32)
                for t in range(GROUP):
                    summed[i, p * GROUP + t] += more[:, t * width : (t + 1) * width]
                return carry

            if arrive is not None:
                lax.fori_loop(0, sets, add_set, 0, unroll=2)

            def place(j, carry, i=i):
                total = summed[i, source[j]] * taken[j]
                ready[j, rows_of(c + i, 1)] = total
                if arrive is not None:
                    squares[j] += total * total
                return carry

            lax.fori_loop(0, slots, place, 0, unroll=8)
        for o in order:
            rows_copy(c, n, o, a_late if arrive is None else a_recv).start()
        mine = ready[pl.ds(shard * slots_dev, slots_dev), rows_of(c, n)]
        out_ref[:, shard, rows_of(c, n), :] = mine

    def late_chunk(c, n):
        if c < SINGLE or c % 2 == 0:
            wait_coded(c, 1 if c < SINGLE else 2)
        finish(c, n, None)

    def own_chunk(c, n):
        if n == 2:
            wait_coded(c, n)
        finish(c, n, lambda: mate_copy(c, n).wait_recv())

    def tell(j, carry):
        for n in range(LATE):
            at = pl.ds(n * PART, PART)
            words, peak = encode([out_ref[j, a, at, :] for a in range(shards)])
            for i, word in enumerate(words):
                late_words[n, j, i] = word
            late_peaks[n, j] = peak
        return carry

    @pl.when(inner)
    def _():
        first_copy.wait()
        for f in range(2):
            far_copy(f).wait()
        pl.semaphore_wait(beyond_sem, 1)
        pl.semaphore_wait(plane_sem, 1)
        done = dict(n=0, f=0, l=0, m=LATE)
        for pattern, times in PLAN:
            now, per = steps(pattern, done)

            def act(k, carry, pattern=pattern, now=now, per=per):
                at = {key: now[key] + k * per[key] for key in now}
                for kind in pattern:
                    n, key = 1 + kind.islower(), kind.lower()
                    if key in "nf":
                        pack(at[key], n, "nf".index(key))
                    elif key == "m":
                        own_chunk(at[key], n)
                    elif key == "l":
                        late_chunk(at[key], n)
                    else:
                        wait_for(others(0, LATE), a_late)
                        lax.fori_loop(0, slots_dev, tell, 0)
                        for copy in back_copies():
                            copy.start()
                    if key in at:
                        at[key] += n
                return carry

            if times == 1:
                act(0, 0)
            else:
                lax.fori_loop(0, times, act, 0)
            done = {key: now[key] + times * per[key] for key in now}
    @pl.when(outer)
    def _():
        pl.semaphore_wait(plane_sem, 1)
        late_copy.wait()

        for n in range(LATE):

            def split(p, carry, n=n):
                at = pl.ds(pl.multiple_of(p * span, span), span)
                rows = late_src[n, :, at].astype(jnp.float32)
                for i in range(GROUP):
                    summed[0, p * GROUP + i] = rows[:, i * width : (i + 1) * width]
                return carry

            lax.fori_loop(0, sets, split, 0, unroll=2)

            def arrange(j, carry, n=n):
                late_mine[n, j] = (summed[0, source[j]] * taken[j]).astype(jnp.bfloat16)
                return carry

            lax.fori_loop(0, slots, arrange, 0, unroll=4)
        for o in order:
            swap_copy(o).start()
        stay_copy.start()
        stay_copy.wait()
        wait_for(late_in.at[pl.ds(0, shards - 1)], lx_recv)
        forward_copy(0).start()

        def own_pair(k, carry):
            c = 2 * k
            finish(c, 2, lambda: mate_copy(c, 2).wait_recv())
            return carry

        def coded_pair(k, carry):
            wait_coded(2 * k, 2)
            return own_pair(k, carry)

        for c, n in pieces(0, 2):
            wait_coded(c, n)
        own_pair(0, 0)
        lax.fori_loop(1, chunks // 2 - 2, coded_pair, 0)
        for copy in back_copies():
            copy.wait_recv()

        def late_squares(j, carry):
            acc = jnp.zeros((PART, width), jnp.float32)
            for n in range(LATE):
                tiles = decode([back_words[n, j, i] for i in range(GROUP // 2 + 1)], back_peaks[n, j])
                for a, tile in enumerate(tiles):
                    total = tile + late_in[a, n, j].astype(jnp.float32)
                    acc += total * total
            squares[shard * slots_dev + j] += acc
            return carry

        lax.fori_loop(0, slots_dev, late_squares, 0)
        lax.fori_loop(chunks // 2 - 2, chunks // 2, coded_pair, 0)

    lane = lax.broadcasted_iota(jnp.int32, (slots, LANES), 1)
    row = lax.broadcasted_iota(jnp.int32, (slots, LANES), 0)
    per_slot = jnp.sum(jnp.sum(squares[...], axis=1), axis=1, keepdims=True)
    total = jnp.sum(jnp.where(lane == row, per_slot, 0.0), axis=0, keepdims=True)

    def grp_copy(o):
        to = lax.rem(grp + o, groups)
        return send(grp_part, grp_all.at[o - 1], g_send, g_recv, (to, shard))

    def shard_copy(o):
        to = flip(shard, o)
        return send(
            shard_part, shard_all.at[o - 1], s_send, s_recv, (grp, to)
        )

    grp_part[...] = total
    for o in range(1, groups):
        grp_copy(o).start()

    @pl.when(outer)
    def _():
        for i in range(1, len(LATE_COPIES)):
            forward_copy(i).start()

    lane = lax.broadcasted_iota(jnp.int32, (1, LANES), 1)

    def lay(j, kinds):
        return jnp.where(lane == j, kind_of[j], kinds)

    kinds = lax.fori_loop(0, slots, lay, jnp.full((1, LANES), 3, jnp.int32))

    wait_for(grp_all, g_recv)
    for o in range(1, groups):
        total = total + grp_all[o - 1]
    shard_part[...] = total
    for o in order:
        shard_copy(o).start()

    @pl.when(inner)
    def _():
        wait_for(out_words, w_send)
        wait_for(out_peaks, p_send)
        wait_for(got, m_send)
        for copy in back_copies():
            copy.wait_send()
        wait_for(others(LATE, chunks), a_recv)

    @pl.when(outer)
    def _():
        wait_for(passed, r_send)
        wait_for(got.at[pl.ds(LATE, chunks - LATE)], m_send)
        wait_for(late_in.at[pl.ds(0, shards - 1)], lx_send)
        wait_for(others(0, chunks), a_recv)

    wait_for(others(0, chunks), a_send)
    wait_for(grp_all, g_send)
    wait_for(shard_all, s_recv)
    wait_for(shard_all, s_send)
    for o in order:
        total = total + shard_all[o - 1]
    total_ref[...] = total
    kinds_ref[...] = kinds

    @pl.when(outer)
    def _():
        wait_for(late_in, lf_send)

    @pl.when(inner)
    def _():
        wait_for(late_raw, lf_recv)


def store_kernel(
    slots_dev,
    in_ref,
    late_ref,
    total_ref,
    kinds_ref,
    out_ref,
    head_ref,
    type_ref,
    late_out,
    heads,
    types,
    sems,
):
    shards = in_ref.shape[1]
    late = pl.ds(0, LATE * PART)
    rest = pl.ds(LATE * PART, in_ref.shape[2] - LATE * PART)
    bulk = [
        pltpu.make_async_copy(in_ref.at[j, :, rest], out_ref.at[j, :, rest], sems.at[0, j])
        for j in range(slots_dev)
    ]
    tops = [
        pltpu.make_async_copy(late_out.at[j], out_ref.at[j, :, late], sems.at[1, j])
        for j in range(slots_dev)
    ]
    small = [
        pltpu.make_async_copy(heads, head_ref, sems.at[2, 0]),
        pltpu.make_async_copy(types, type_ref, sems.at[2, 1]),
    ]
    for copy in bulk:
        copy.start()
    grp, shard = lax.axis_index("grp"), lax.axis_index("shard")
    inner = (grp > 0) & (grp < lax.axis_size("grp") - 1)
    for j in range(slots_dev):

        def add_late(a, carry, j=j):
            for c in range(LATE):
                at = pl.ds(c * PART, PART)
                more = jnp.where(inner, late_ref[a, c, j].astype(jnp.float32), 0.0)
                late_out[j, a, at, :] = in_ref[j, a, at, :] + more
            return carry

        lax.fori_loop(0, shards, add_late, 0, unroll=True)
        tops[j].start()
    total = total_ref[...]
    kinds = kinds_ref[...]
    lane = lax.broadcasted_iota(jnp.int32, (1, LANES), 1)
    root = jnp.sqrt(total / (D * HS))
    for i in range(slots_dev):
        heads[i] = jnp.sum(jnp.where(lane == shard * slots_dev + i, root, 0.0))
    for t, count in enumerate((QH, KVH, KVH)):
        one = jnp.sum(jnp.where(kinds == t, total, 0.0), axis=1, keepdims=True)
        types[t] = jnp.sum(jnp.sqrt(one / (count * D * HS)))
    for copy in small:
        copy.start()
    for copy in bulk + tops + small:
        copy.wait()


def line_step(x, joined, slot, blocks, slots_dev, shards, rows, width):
    chunks = rows // PART
    cols = blocks * width
    sets = blocks // GROUP
    slots = slots_dev * shards
    half = GROUP // 2
    dma = pltpu.SemaphoreType.DMA
    regular = pltpu.SemaphoreType.REGULAR
    f32, i32, bf16 = jnp.float32, jnp.int32, jnp.bfloat16
    out, late, total, kinds = pl.pallas_call(
        functools.partial(line_kernel, blocks, slots_dev),
        out_shape=[
            pltpu.VMEM((slots_dev, shards, rows, width), f32),
            pltpu.VMEM((shards, LATE, slots_dev, PART, width), bf16),
            pltpu.VMEM((1, LANES), f32),
            pltpu.VMEM((1, LANES), i32),
        ],
        in_specs=[pl.BlockSpec(memory_space=pltpu.HBM)] * 3,
        out_specs=[pl.BlockSpec(memory_space=pltpu.VMEM)] * 4,
        scratch_shapes=[
            pltpu.SMEM((blocks,), i32),
            pltpu.SMEM((blocks,), i32),
            pltpu.VMEM((1, PART, cols), bf16),
            pltpu.VMEM((chunks, PART, cols), bf16),
            pltpu.VMEM((2, chunks, PART, cols), bf16),
            pltpu.VMEM((2, chunks, PART, cols), bf16),
            pltpu.VMEM((chunks, PART, cols), bf16),
            pltpu.VMEM((2, chunks, sets, half + 1, PART, width), i32),
            pltpu.VMEM((2, chunks, sets, 1, width), f32),
            pltpu.VMEM((chunks, sets, half + 1, PART, width), i32),
            pltpu.VMEM((chunks, sets, 1, width), f32),
            pltpu.VMEM((slots, rows, width), f32),
            pltpu.VMEM((LATE, PART, cols), bf16),
            pltpu.VMEM((LATE, slots, PART, width), bf16),
            pltpu.VMEM((shards, LATE, slots_dev, PART, width), bf16),
            pltpu.VMEM((LATE, slots_dev, half + 1, PART, width), i32),
            pltpu.VMEM((LATE, slots_dev, 1, width), f32),
            pltpu.VMEM((LATE, slots_dev, half + 1, PART, width), i32),
            pltpu.VMEM((LATE, slots_dev, 1, width), f32),
            pltpu.SMEM((slots,), i32),
            pltpu.SMEM((slots,), f32),
            pltpu.SMEM((slots,), i32),
            pltpu.VMEM((2, blocks, PART, width), f32),
            pltpu.VMEM((slots, PART, width), f32),
            pltpu.VMEM((1, LANES), f32),
            pltpu.VMEM((3, 1, LANES), f32),
            pltpu.VMEM((1, LANES), f32),
            pltpu.VMEM((shards - 1, 1, LANES), f32),
            dma((2,)),
            dma,
            dma,
            dma((2,)),
            regular,
            regular,
            dma,
            dma((len(pieces(0, chunks)), 2)),
            dma,
            dma((chunks // 2,)),
            dma,
            dma((len(pieces(0, chunks)),)),
            dma,
            dma((len(pieces(0, chunks)),)),
            dma,
            dma,
            dma,
            dma,
            dma,
            dma,
            dma,
            dma,
            dma,
            dma,
            dma,
            dma,
            dma,
            dma((2,)),
            dma((2,)),
        ],
        compiler_params=pltpu.CompilerParams(
            collective_id=0,
            has_side_effects=True,
            vmem_limit_bytes=57 * 1024 * 1024,
        ),
    )(x.reshape(4 * chunks, PART, cols), joined, slot)
    return pl.pallas_call(
        functools.partial(store_kernel, slots_dev),
        out_shape=[
            jax.ShapeDtypeStruct((slots_dev, shards, rows, width), f32),
            jax.ShapeDtypeStruct((slots_dev,), f32),
            jax.ShapeDtypeStruct((3,), f32),
        ],
        in_specs=[pl.BlockSpec(memory_space=pltpu.VMEM)] * 4,
        out_specs=[pl.BlockSpec(memory_space=pltpu.HBM)] * 3,
        scratch_shapes=[
            pltpu.VMEM((slots_dev, shards, LATE * PART, width), f32),
            pltpu.SMEM((slots_dev,), f32),
            pltpu.SMEM((3,), f32),
            dma((3, slots_dev)),
        ],
        compiler_params=pltpu.CompilerParams(vmem_limit_bytes=4 * 1024 * 1024),
    )(out, late, total, kinds)


def any_kernel(groups, shards, blocks, slots_dev, chunks, *refs):
    x_ref, joined_ref, slot_ref = refs[:3]
    out_ref, head_ref, type_ref = refs[3:6]
    own = refs[6]
    got = refs[7 : 7 + chunks]
    ready = refs[7 + chunks : 7 + 2 * chunks]
    rest = refs[7 + 2 * chunks :]
    (source, taken, kind_of, summed, squares, shard_part, shard_all, grp_part, grp_all) = rest[:9]
    (own_sem, z_send, z_recv, a_send, a_recv, keep_sem, s_send, s_recv, g_send, g_recv) = rest[9:]

    grp = lax.axis_index("grp")
    shard = lax.axis_index("shard")
    slots = slots_dev * shards
    rows = own.shape[0]
    part = rows // chunks
    width = own.shape[1] // blocks

    def grp_peer(offset):
        return lax.rem(grp + offset, groups)

    def shard_peer(offset):
        return lax.rem(shard + offset, shards)

    load_own = pltpu.make_async_copy(
        x_ref.at[0, pl.ds(pl.multiple_of(grp * rows, 8), rows), :], own, own_sem
    )
    load_own.start()

    barrier = pltpu.get_barrier_semaphore()
    for o in range(1, groups):
        pl.semaphore_signal(barrier, 1, device_id=(grp_peer(o), shard), device_id_type=MESH)
    for o in range(1, shards):
        pl.semaphore_signal(barrier, 1, device_id=(grp, shard_peer(o)), device_id_type=MESH)
    pl.semaphore_wait(barrier, groups + shards - 2)

    z_copies = []
    for c in range(chunks):
        for o in range(1, groups):
            first = pl.multiple_of(grp_peer(o) * rows + c * part, 8)
            copy = pltpu.make_async_remote_copy(
                src_ref=x_ref.at[0, pl.ds(first, part), :],
                dst_ref=got[c].at[o - 1],
                send_sem=z_send.at[c, o - 1],
                recv_sem=z_recv.at[c, o - 1],
                device_id=(grp_peer(o), shard),
                device_id_type=MESH,
            )
            copy.start()
            z_copies.append(copy)

    def find(j, carry):
        found, block, kind = jnp.float32(0), jnp.int32(0), jnp.int32(3)
        for b in range(blocks):
            hit = slot_ref[b] == j
            found = jnp.where(hit, 1.0, found)
            block = jnp.where(hit, joined_ref[b], block)
            kind = jnp.where(hit, (b >= QH) + (b >= QH + KVH), kind)
        source[j] = block
        taken[j] = found
        kind_of[j] = kind
        return carry

    lax.fori_loop(0, slots, find, 0)

    load_own.wait()
    a_copies = []
    for c in range(chunks):
        for o in range(1, groups):
            z_copies[c * (groups - 1) + o - 1].wait_recv()

        def add(k, carry):
            at = pl.multiple_of(k * width, width)
            total = own[c * part : (c + 1) * part, pl.ds(at, width)].astype(jnp.float32)
            for o in range(1, groups):
                total += got[c][o - 1, :, pl.ds(at, width)].astype(jnp.float32)
            summed[k] = total
            return carry

        lax.fori_loop(0, blocks, add, 0, unroll=4)

        def slot(j, carry):
            total = summed[source[j]] * taken[j]
            ready[c][j] = total
            sq = jnp.sum((total * total).reshape(part // 8, 8, width), axis=0)
            squares[j] = sq if c == 0 else squares[j] + sq
            return carry

        lax.fori_loop(0, slots, slot, 0, unroll=4)

        if c == chunks - 1:
            lane = lax.broadcasted_iota(jnp.int32, (slots, LANES), 1)
            row = lax.broadcasted_iota(jnp.int32, (slots, LANES), 0)
            per_slot = jnp.sum(jnp.sum(squares[...], axis=1), axis=1, keepdims=True)
            shard_part[...] = jnp.sum(jnp.where(lane == row, per_slot, 0.0), axis=0, keepdims=True)
            s_copies = []
            for o in range(1, shards):
                copy = pltpu.make_async_remote_copy(
                    src_ref=shard_part,
                    dst_ref=shard_all.at[o - 1],
                    send_sem=s_send.at[o - 1],
                    recv_sem=s_recv.at[o - 1],
                    device_id=(grp, shard_peer(o)),
                    device_id_type=MESH,
                )
                copy.start()
                s_copies.append(copy)

        for o in range(1, shards):
            copy = pltpu.make_async_remote_copy(
                src_ref=ready[c].at[pl.ds(shard_peer(o) * slots_dev, slots_dev)],
                dst_ref=out_ref.at[:, shard, pl.ds(c * part, part), :],
                send_sem=a_send.at[c, o - 1],
                recv_sem=a_recv.at[c, o - 1],
                device_id=(grp, shard_peer(o)),
                device_id_type=MESH,
            )
            copy.start()
            a_copies.append(copy)
        copy = pltpu.make_async_copy(
            ready[c].at[pl.ds(shard * slots_dev, slots_dev)],
            out_ref.at[:, shard, pl.ds(c * part, part), :],
            keep_sem.at[c],
        )
        copy.start()
        a_copies.append(copy)

    total = shard_part[...]
    for o in range(1, shards):
        s_copies[o - 1].wait()
        total = total + shard_all[o - 1]
    grp_part[...] = total
    g_copies = []
    for o in range(1, groups):
        copy = pltpu.make_async_remote_copy(
            src_ref=grp_part,
            dst_ref=grp_all.at[o - 1],
            send_sem=g_send.at[o - 1],
            recv_sem=g_recv.at[o - 1],
            device_id=(grp_peer(o), shard),
            device_id_type=MESH,
        )
        copy.start()
        g_copies.append(copy)
    lane = lax.broadcasted_iota(jnp.int32, (1, LANES), 1)

    def lay(j, kinds):
        return jnp.where(lane == j, kind_of[j], kinds)

    kinds = lax.fori_loop(0, slots, lay, jnp.full((1, LANES), 3, jnp.int32))
    for o in range(1, groups):
        g_copies[o - 1].wait()
        total = total + grp_all[o - 1]
    root = jnp.sqrt(total / (D * HS))
    for i in range(slots_dev):
        head_ref[i] = jnp.sum(jnp.where(lane == shard * slots_dev + i, root, 0.0))
    for t, heads in enumerate((QH, KVH, KVH)):
        one = jnp.sum(jnp.where(kinds == t, total, 0.0), axis=1, keepdims=True)
        type_ref[t] = jnp.sum(jnp.sqrt(one / (heads * D * HS)))

    for copy in z_copies:
        copy.wait_send()
    for copy in a_copies:
        copy.wait()


def any_step(x, joined, slot, groups, shards, blocks, slots_dev, rows, width):
    slots = slots_dev * shards
    cols = blocks * width
    part = chunk_rows(rows)
    chunks = rows // part
    dma = pltpu.SemaphoreType.DMA
    return pl.pallas_call(
        functools.partial(any_kernel, groups, shards, blocks, slots_dev, chunks),
        out_shape=[
            jax.ShapeDtypeStruct((slots_dev, shards, rows, width), jnp.float32),
            jax.ShapeDtypeStruct((slots_dev,), jnp.float32),
            jax.ShapeDtypeStruct((3,), jnp.float32),
        ],
        in_specs=[
            pl.BlockSpec(memory_space=pltpu.HBM),
            pl.BlockSpec(memory_space=pltpu.SMEM),
            pl.BlockSpec(memory_space=pltpu.SMEM),
        ],
        out_specs=[
            pl.BlockSpec(memory_space=pl.ANY),
            pl.BlockSpec(memory_space=pltpu.SMEM),
            pl.BlockSpec(memory_space=pltpu.SMEM),
        ],
        scratch_shapes=[pltpu.VMEM((rows, cols), jnp.bfloat16)]
        + [pltpu.VMEM((groups - 1, part, cols), jnp.bfloat16)] * chunks
        + [pltpu.VMEM((slots, part, width), jnp.float32)] * chunks
        + [
            pltpu.SMEM((slots,), jnp.int32),
            pltpu.SMEM((slots,), jnp.float32),
            pltpu.SMEM((slots,), jnp.int32),
            pltpu.VMEM((blocks, part, width), jnp.float32),
            pltpu.VMEM((slots, 8, width), jnp.float32),
            pltpu.VMEM((1, LANES), jnp.float32),
            pltpu.VMEM((shards - 1, 1, LANES), jnp.float32),
            pltpu.VMEM((1, LANES), jnp.float32),
            pltpu.VMEM((groups - 1, 1, LANES), jnp.float32),
            dma,
            dma((chunks, groups - 1)),
            dma((chunks, groups - 1)),
            dma((chunks, shards - 1)),
            dma((chunks, shards - 1)),
            dma((chunks,)),
            dma((shards - 1,)),
            dma((shards - 1,)),
            dma((groups - 1,)),
            dma((groups - 1,)),
        ],
        compiler_params=pltpu.CompilerParams(
            collective_id=0,
            has_side_effects=True,
            vmem_limit_bytes=60 * 1024 * 1024,
        ),
    )(x, joined, slot)


def solution(mesh):
    groups, shards = mesh.shape["grp"], mesh.shape["shard"]

    def step(x, joined, slot):
        blocks = joined.shape[0]
        slots_dev = (blocks + shards - 1) // shards
        rows = x.shape[1] // groups
        width = x.shape[2] // blocks
        line = groups == 4 and shards == 8 and rows == 16 * PART and blocks % GROUP == 0
        if line and width == LANES and slots_dev * shards <= LANES:
            return tuple(line_step(x, joined, slot, blocks, slots_dev, shards, rows, width))
        return tuple(any_step(x, joined, slot, groups, shards, blocks, slots_dev, rows, width))

    return jax.shard_map(
        step,
        mesh=mesh,
        in_specs=(P("grp", "shard", None), P(), P()),
        out_specs=(P("shard", None, "grp", None), P("shard"), P()),
        check_vma=False,
    )
```

```python
import functools

import jax
import jax.numpy as jnp
from jax import lax
from jax.experimental import pallas as pl
from jax.experimental.pallas import tpu as pltpu
from jax.sharding import PartitionSpec as P

D = 4096
QH = 32
KVH = 8
HS = 128
LANES = 128
MESH = pl.DeviceIdType.MESH


def chunk_rows(rows):
    return 16 if rows % 16 == 0 else rows


PART = 8
GROUP = 8
BITS = 19
QMAX = (1 - 2.0**-10) * 2.0 ** (BITS - 2)
SMALL = 2.0**-120
LATE = 5
LATE_COPIES = ((0, 1), (1, 2), (3, 2))
SINGLE = 2
PLAN = (("FNFNLfnLflnfnLMfAnm", 1), ("fnm", 3), ("m", 1))
AHEAD = 4


def pieces(first, last):
    c, found = first, []
    while c < last:
        n = 2 if c % 2 == 0 and c + 2 <= last and c >= SINGLE else 1
        found.append((c, n))
        c += n
    return found


def powers(e):
    half = e >> 1
    return jnp.exp2(half.astype(jnp.float32)), jnp.exp2((e - half).astype(jnp.float32))


def encode(tiles):
    peak = functools.reduce(jnp.maximum, [jnp.abs(t) for t in tiles])
    e = jnp.ceil(jnp.log2(jnp.maximum(peak, SMALL))).astype(jnp.int32) - 1
    p, q = powers(-e)
    p = p * QMAX
    codes = [jnp.round(t * q * p).astype(jnp.int32) for t in tiles]
    half, low = GROUP // 2, 32 - BITS
    high = BITS - low
    words = [(codes[i] << low) | (codes[half + i] & ((1 << low) - 1)) for i in range(half)]
    last = e << 24
    for i in range(half):
        last |= ((codes[half + i] >> low) & ((1 << high) - 1)) << (high * i)
    return words + [last]


def decode(words):
    half, low = GROUP // 2, 32 - BITS
    high = BITS - low
    p, q = powers(words[half] >> 24)
    p = p * (1.0 / QMAX)
    codes = [words[i] >> low for i in range(half)]
    for i in range(half):
        top = (words[half] << (32 - high * (i + 1))) >> (32 - high)
        codes.append((top << low) | (words[i] & ((1 << low) - 1)))
    return [c.astype(jnp.float32) * p * q for c in codes]


def piece(c, n):
    return c if n == 1 else lax.div(c, 2) + SINGLE // 2


def wait_for(ref, sem):
    pltpu.make_async_copy(ref, ref, sem).wait()


def steps(pattern, done):
    per = {k: sum(1 + c.islower() for c in pattern if c.lower() == k) for k in done}
    return dict(done), per


def flip(s, o):
    for b in range(3):
        if o >> b & 1:
            s = s + (1 - 2 * lax.rem(lax.div(s, 1 << b), 2)) * (1 << b)
    return s


def line_kernel(
    blocks,
    slots_dev,
    x_ref,
    joined_hbm,
    slot_hbm,
    out_ref,
    late_raw,
    total_ref,
    kinds_ref,
    joined_ref,
    slot_ref,
    first,
    own,
    far,
    passed,
    got,
    out_words,
    in_words,
    ready,
    late_src,
    late_mine,
    late_in,
    late_words,
    back_words,
    source,
    taken,
    kind_of,
    summed,
    squares,
    grp_part,
    grp_all,
    shard_part,
    shard_all,
    index_sem,
    first_sem,
    own_sem,
    far_sem,
    plane_sem,
    beyond_sem,
    r_send,
    r_recv,
    m_send,
    m_recv,
    w_send,
    w_recv,
    a_send,
    a_recv,
    a_late,
    g_send,
    g_recv,
    s_send,
    s_recv,
    late_sem,
    lx_send,
    lx_recv,
    lk_sem,
    lf_send,
    lf_recv,
    la_send,
    la_recv,
):
    groups, shards = 4, 8
    grp = lax.axis_index("grp")
    shard = lax.axis_index("shard")
    slots = slots_dev * shards
    chunks = own.shape[0]
    width = own.shape[2] // blocks
    sets = blocks // GROUP
    span = GROUP * width

    outer = (grp == 0) | (grp == groups - 1)
    inner = jnp.logical_not(outer)
    mate = grp + 1 - 2 * lax.rem(grp, 2)
    near = jnp.where(outer, 3 - mate, 3 - grp)
    beyond = near + 1 - 2 * lax.rem(near, 2)
    dests = (near, beyond)

    own_copy = pltpu.make_async_copy(x_ref.at[pl.ds(grp * chunks, chunks)], own, own_sem)

    def far_copy(f):
        return pltpu.make_async_copy(
            x_ref.at[pl.ds(dests[f] * chunks, chunks)], far.at[f], far_sem.at[f]
        )

    def send(src, dst, send_sem, recv_sem, to):
        return pltpu.make_async_remote_copy(
            src_ref=src,
            dst_ref=dst,
            send_sem=send_sem,
            recv_sem=recv_sem,
            device_id=to,
            device_id_type=MESH,
        )

    index_copies = [
        pltpu.make_async_copy(joined_hbm, joined_ref, index_sem.at[0]),
        pltpu.make_async_copy(slot_hbm, slot_ref, index_sem.at[1]),
    ]
    first_copy = pltpu.make_async_copy(x_ref.at[pl.ds(beyond * chunks, 1)], first, first_sem)

    def relay_copy(c, n, f):
        staged = isinstance(c, int) and c == 0 and f == 1
        src = first if staged else x_ref.at[pl.ds(dests[f] * chunks + c, n)]
        dst = passed.at[f, pl.ds(c, n)]
        return send(src, dst, r_send, r_recv.at[piece(c, n), f], (mate, shard))

    def mate_copy(c, n):
        src = x_ref.at[pl.ds(mate * chunks + c, n)]
        return send(src, got.at[pl.ds(c, n)], m_send, m_recv.at[lax.div(c, 2)], (mate, shard))

    def coded_copy(c, n, f):
        at = pl.ds(c, n)
        to = (dests[f], shard)
        return send(out_words.at[f, at], in_words.at[at], w_send, w_recv.at[piece(c, n)], to)

    order = (6, 7, 2, 4, 3, 5, 1)

    def rows_of(c, n):
        return pl.ds(pl.multiple_of(c * PART, PART), n * PART)

    def rows_copy(c, n, o, recv_sem):
        to = flip(shard, o)
        return send(
            ready.at[pl.ds(to * slots_dev, slots_dev), rows_of(c, n)],
            out_ref.at[:, shard, rows_of(c, n), :],
            a_send,
            recv_sem,
            (grp, to),
        )

    def others(first, last):
        at = pl.ds(first * PART, (last - first) * PART)
        return ready.at[pl.ds(0, (shards - 1) * slots_dev), at]

    late_copy = pltpu.make_async_copy(x_ref.at[pl.ds(mate * chunks, LATE)], late_src, late_sem)

    def swap_copy(o):
        to = flip(shard, o)
        return send(
            late_mine.at[:, pl.ds(to * slots_dev, slots_dev)],
            late_in.at[shard],
            lx_send,
            lx_recv,
            (grp, to),
        )

    stay_copy = pltpu.make_async_copy(
        late_mine.at[:, pl.ds(shard * slots_dev, slots_dev)], late_in.at[shard], lk_sem
    )

    def forward_copy(i):
        at = pl.ds(*LATE_COPIES[i])
        to = (mate, shard)
        return send(late_in.at[:, at], late_raw.at[:, at], lf_send, lf_recv, to)

    back_copy = send(late_words, back_words, la_send, la_recv, (mate, shard))

    first_copy.start()

    barrier = pltpu.get_barrier_semaphore()
    pl.semaphore_signal(barrier, 1, device_id=(mate, shard), device_id_type=MESH)
    for o in range(1, 6):
        pl.semaphore_signal(barrier, 1, device_id=(grp, flip(shard, o)), device_id_type=MESH)

    @pl.when(inner)
    def _():
        pl.semaphore_signal(barrier, 1, device_id=(near, shard), device_id_type=MESH)
        pl.semaphore_wait(barrier, 7)
        own_copy.start()
        pl.semaphore_signal(beyond_sem, 1, device_id=(near, shard), device_id_type=MESH)
        for f in range(2):
            far_copy(f).start()
        for c in range(0, AHEAD, 2):
            mate_copy(c, 2).start()

    @pl.when(outer)
    def _():
        pl.semaphore_wait(barrier, 6)
        first_copy.wait()
        done = dict(n=0, f=0, m=LATE)
        for pattern, times in PLAN:
            now, per = steps(pattern, done)

            def queue(k, carry, pattern=pattern, now=now, per=per):
                at = {key: now[key] + k * per[key] for key in now}
                for kind in pattern:
                    n, key = 1 + kind.islower(), kind.lower()
                    if key in "nf":
                        relay_copy(at[key], n, "nf".index(key)).start()
                    elif key == "m":
                        mate_copy(at[key], n).start()
                    if key in at:
                        at[key] += n
                return carry

            if times == 1:
                queue(0, 0)
            else:
                lax.fori_loop(0, times, queue, 0)
            done = {key: now[key] + times * per[key] for key in now}
        own_copy.start()
        late_copy.start()

    pl.semaphore_signal(plane_sem, 1, device_id=(grp, flip(shard, 2)), device_id_type=MESH)

    def find(j, carry):
        head = jnp.int32(-1)
        for b in range(blocks):
            head = jnp.where(slot_ref[b] == j, b, head)
        there = head >= 0
        source[j] = jnp.where(there, joined_ref[jnp.maximum(head, 0)], 0)
        taken[j] = jnp.where(there, 1.0, 0.0)
        kind = jnp.where(head >= QH, 1, 0) + jnp.where(head >= QH + KVH, 1, 0)
        kind_of[j] = jnp.where(there, kind, 3)
        return carry

    for copy in index_copies:
        copy.start()
    for copy in index_copies:
        copy.wait()
    lax.fori_loop(0, slots, find, 0)
    own_copy.wait()

    def clear(j, carry):
        squares[j] = jnp.zeros((PART, width), jnp.float32)
        return carry

    lax.fori_loop(0, slots, clear, 0)

    def pack(c, n, f):
        relay_copy(c, n, f).wait_recv()

        def pack_set(q, carry):
            i, p = lax.div(q, sets), lax.rem(q, sets)
            at = pl.ds(pl.multiple_of(p * span, span), span)
            total = far[f, c + i, :, at].astype(jnp.float32)
            total += passed[f, c + i, :, at].astype(jnp.float32)
            words = encode([total[:, i * width : (i + 1) * width] for i in range(GROUP)])
            for w, word in enumerate(words):
                out_words[f, c + i, p, w] = word
            return carry

        lax.fori_loop(0, n * sets, pack_set, 0, unroll=2)
        coded_copy(c, n, f).start()
        if f == 1 and n == 2:

            @pl.when(c + AHEAD - SINGLE < chunks)
            def _():
                mate_copy(c + AHEAD - SINGLE, 2).start()

    def wait_coded(c, n):
        coded_copy(c, n, 0).wait_recv()

    def finish(c, n, arrive):
        for i in range(n):

            def pre_set(p, carry, i=i):
                at = pl.ds(pl.multiple_of(p * span, span), span)
                mine = own[c + i, :, at].astype(jnp.float32)
                words = [in_words[c + i, p, w] for w in range(GROUP // 2 + 1)]
                for t, tile in enumerate(decode(words)):
                    summed[i, p * GROUP + t] = mine[:, t * width : (t + 1) * width] + tile
                return carry

            lax.fori_loop(0, sets, pre_set, 0, unroll=2)
        if arrive is not None:
            arrive()
        for i in range(n):

            def add_set(p, carry, i=i):
                at = pl.ds(pl.multiple_of(p * span, span), span)
                more = got[c + i, :, at].astype(jnp.float32)
                for t in range(GROUP):
                    summed[i, p * GROUP + t] += more[:, t * width : (t + 1) * width]
                return carry

            if arrive is not None:
                lax.fori_loop(0, sets, add_set, 0, unroll=2)

            def place(j, carry, i=i):
                total = summed[i, source[j]] * taken[j]
                ready[j, rows_of(c + i, 1)] = total
                if arrive is not None:
                    squares[j] += total * total
                return carry

            lax.fori_loop(0, slots, place, 0, unroll=8)
        for o in order:
            rows_copy(c, n, o, a_late if arrive is None else a_recv).start()
        mine = ready[pl.ds(shard * slots_dev, slots_dev), rows_of(c, n)]
        out_ref[:, shard, rows_of(c, n), :] = mine

    def late_chunk(c, n):
        if c < SINGLE or c % 2 == 0:
            wait_coded(c, 1 if c < SINGLE else 2)
        finish(c, n, None)

    def own_chunk(c, n):
        if n == 2:
            wait_coded(c, n)
        finish(c, n, lambda: mate_copy(c, n).wait_recv())

    def tell(j, carry):
        for n in range(LATE):
            at = pl.ds(n * PART, PART)
            words = encode([out_ref[j, a, at, :] for a in range(shards)])
            for i, word in enumerate(words):
                late_words[n, j, i] = word
        return carry

    @pl.when(inner)
    def _():
        first_copy.wait()
        for f in range(2):
            far_copy(f).wait()
        pl.semaphore_wait(beyond_sem, 1)
        pl.semaphore_wait(plane_sem, 1)
        done = dict(n=0, f=0, l=0, m=LATE)
        for pattern, times in PLAN:
            now, per = steps(pattern, done)

            def act(k, carry, pattern=pattern, now=now, per=per):
                at = {key: now[key] + k * per[key] for key in now}
                for kind in pattern:
                    n, key = 1 + kind.islower(), kind.lower()
                    if key in "nf":
                        pack(at[key], n, "nf".index(key))
                    elif key == "m":
                        own_chunk(at[key], n)
                    elif key == "l":
                        late_chunk(at[key], n)
                    else:
                        wait_for(others(0, LATE), a_late)
                        lax.fori_loop(0, slots_dev, tell, 0)
                        back_copy.start()
                    if key in at:
                        at[key] += n
                return carry

            if times == 1:
                act(0, 0)
            else:
                lax.fori_loop(0, times, act, 0)
            done = {key: now[key] + times * per[key] for key in now}
    @pl.when(outer)
    def _():
        pl.semaphore_wait(plane_sem, 1)
        late_copy.wait()

        for n in range(LATE):

            def split(p, carry, n=n):
                at = pl.ds(pl.multiple_of(p * span, span), span)
                rows = late_src[n, :, at].astype(jnp.float32)
                for i in range(GROUP):
                    summed[0, p * GROUP + i] = rows[:, i * width : (i + 1) * width]
                return carry

            lax.fori_loop(0, sets, split, 0, unroll=2)

            def arrange(j, carry, n=n):
                late_mine[n, j] = (summed[0, source[j]] * taken[j]).astype(jnp.bfloat16)
                return carry

            lax.fori_loop(0, slots, arrange, 0, unroll=4)
        for o in order:
            swap_copy(o).start()
        stay_copy.start()
        stay_copy.wait()
        wait_for(late_in.at[pl.ds(0, shards - 1)], lx_recv)
        forward_copy(0).start()

        def own_pair(k, carry):
            c = 2 * k
            finish(c, 2, lambda: mate_copy(c, 2).wait_recv())
            return carry

        def coded_pair(k, carry):
            wait_coded(2 * k, 2)
            return own_pair(k, carry)

        for c, n in pieces(0, 2):
            wait_coded(c, n)
        own_pair(0, 0)
        lax.fori_loop(1, chunks // 2 - 2, coded_pair, 0)
        back_copy.wait_recv()

        def late_squares(j, carry):
            acc = jnp.zeros((PART, width), jnp.float32)
            for n in range(LATE):
                tiles = decode([back_words[n, j, i] for i in range(GROUP // 2 + 1)])
                for a, tile in enumerate(tiles):
                    total = tile + late_in[a, n, j].astype(jnp.float32)
                    acc += total * total
            squares[shard * slots_dev + j] += acc
            return carry

        lax.fori_loop(0, slots_dev, late_squares, 0)
        lax.fori_loop(chunks // 2 - 2, chunks // 2, coded_pair, 0)

    lane = lax.broadcasted_iota(jnp.int32, (slots, LANES), 1)
    row = lax.broadcasted_iota(jnp.int32, (slots, LANES), 0)
    per_slot = jnp.sum(jnp.sum(squares[...], axis=1), axis=1, keepdims=True)
    total = jnp.sum(jnp.where(lane == row, per_slot, 0.0), axis=0, keepdims=True)

    def grp_copy(o):
        to = lax.rem(grp + o, groups)
        return send(grp_part, grp_all.at[o - 1], g_send, g_recv, (to, shard))

    def shard_copy(o):
        to = flip(shard, o)
        return send(
            shard_part, shard_all.at[o - 1], s_send, s_recv, (grp, to)
        )

    grp_part[...] = total
    for o in range(1, groups):
        grp_copy(o).start()

    @pl.when(outer)
    def _():
        for i in range(1, len(LATE_COPIES)):
            forward_copy(i).start()

    lane = lax.broadcasted_iota(jnp.int32, (1, LANES), 1)

    def lay(j, kinds):
        return jnp.where(lane == j, kind_of[j], kinds)

    kinds = lax.fori_loop(0, slots, lay, jnp.full((1, LANES), 3, jnp.int32))

    wait_for(grp_all, g_recv)
    for o in range(1, groups):
        total = total + grp_all[o - 1]
    shard_part[...] = total
    for o in order:
        shard_copy(o).start()

    @pl.when(inner)
    def _():
        wait_for(out_words, w_send)
        wait_for(got, m_send)
        back_copy.wait_send()
        wait_for(others(LATE, chunks), a_recv)

    @pl.when(outer)
    def _():
        wait_for(passed, r_send)
        wait_for(got.at[pl.ds(LATE, chunks - LATE)], m_send)
        wait_for(late_in.at[pl.ds(0, shards - 1)], lx_send)
        wait_for(others(0, chunks), a_recv)

    wait_for(others(0, chunks), a_send)
    wait_for(grp_all, g_send)
    wait_for(shard_all, s_recv)
    wait_for(shard_all, s_send)
    for o in order:
        total = total + shard_all[o - 1]
    total_ref[...] = total
    kinds_ref[...] = kinds

    @pl.when(outer)
    def _():
        wait_for(late_in, lf_send)

    @pl.when(inner)
    def _():
        wait_for(late_raw, lf_recv)


def store_kernel(
    slots_dev,
    in_ref,
    late_ref,
    total_ref,
    kinds_ref,
    out_ref,
    head_ref,
    type_ref,
    late_out,
    heads,
    types,
    sems,
):
    shards = in_ref.shape[1]
    late = pl.ds(0, LATE * PART)
    rest = pl.ds(LATE * PART, in_ref.shape[2] - LATE * PART)
    bulk = [
        pltpu.make_async_copy(in_ref.at[j, :, rest], out_ref.at[j, :, rest], sems.at[0])
        for j in range(slots_dev)
    ]
    tops = [
        pltpu.make_async_copy(late_out.at[j], out_ref.at[j, :, late], sems.at[0])
        for j in range(slots_dev)
    ]
    small = [
        pltpu.make_async_copy(heads, head_ref, sems.at[1]),
        pltpu.make_async_copy(types, type_ref, sems.at[2]),
    ]
    for copy in bulk:
        copy.start()
    grp, shard = lax.axis_index("grp"), lax.axis_index("shard")
    inner = (grp > 0) & (grp < lax.axis_size("grp") - 1)
    for j in range(slots_dev):

        def add_late(a, carry, j=j):
            for c in range(LATE):
                at = pl.ds(c * PART, PART)
                more = jnp.where(inner, late_ref[a, c, j].astype(jnp.float32), 0.0)
                late_out[j, a, at, :] = in_ref[j, a, at, :] + more
            return carry

        lax.fori_loop(0, shards, add_late, 0, unroll=True)
        tops[j].start()
    total = total_ref[...]
    kinds = kinds_ref[...]
    lane = lax.broadcasted_iota(jnp.int32, (1, LANES), 1)
    root = jnp.sqrt(total / (D * HS))
    for i in range(slots_dev):
        heads[i] = jnp.sum(jnp.where(lane == shard * slots_dev + i, root, 0.0))
    for t, count in enumerate((QH, KVH, KVH)):
        one = jnp.sum(jnp.where(kinds == t, total, 0.0), axis=1, keepdims=True)
        types[t] = jnp.sum(jnp.sqrt(one / (count * D * HS)))
    for copy in small:
        copy.start()
    for copy in small:
        copy.wait()
    wait_for(out_ref, sems.at[0])


def line_step(x, joined, slot, blocks, slots_dev, shards, rows, width):
    chunks = rows // PART
    cols = blocks * width
    sets = blocks // GROUP
    slots = slots_dev * shards
    half = GROUP // 2
    dma = pltpu.SemaphoreType.DMA
    regular = pltpu.SemaphoreType.REGULAR
    f32, i32, bf16 = jnp.float32, jnp.int32, jnp.bfloat16
    out, late, total, kinds = pl.pallas_call(
        functools.partial(line_kernel, blocks, slots_dev),
        out_shape=[
            pltpu.VMEM((slots_dev, shards, rows, width), f32),
            pltpu.VMEM((shards, LATE, slots_dev, PART, width), bf16),
            pltpu.VMEM((1, LANES), f32),
            pltpu.VMEM((1, LANES), i32),
        ],
        in_specs=[pl.BlockSpec(memory_space=pltpu.HBM)] * 3,
        out_specs=[pl.BlockSpec(memory_space=pltpu.VMEM)] * 4,
        scratch_shapes=[
            pltpu.SMEM((blocks,), i32),
            pltpu.SMEM((blocks,), i32),
            pltpu.VMEM((1, PART, cols), bf16),
            pltpu.VMEM((chunks, PART, cols), bf16),
            pltpu.VMEM((2, chunks, PART, cols), bf16),
            pltpu.VMEM((2, chunks, PART, cols), bf16),
            pltpu.VMEM((chunks, PART, cols), bf16),
            pltpu.VMEM((2, chunks, sets, half + 1, PART, width), i32),
            pltpu.VMEM((chunks, sets, half + 1, PART, width), i32),
            pltpu.VMEM((slots, rows, width), f32),
            pltpu.VMEM((LATE, PART, cols), bf16),
            pltpu.VMEM((LATE, slots, PART, width), bf16),
            pltpu.VMEM((shards, LATE, slots_dev, PART, width), bf16),
            pltpu.VMEM((LATE, slots_dev, half + 1, PART, width), i32),
            pltpu.VMEM((LATE, slots_dev, half + 1, PART, width), i32),
            pltpu.SMEM((slots,), i32),
            pltpu.SMEM((slots,), f32),
            pltpu.SMEM((slots,), i32),
            pltpu.VMEM((2, blocks, PART, width), f32),
            pltpu.VMEM((slots, PART, width), f32),
            pltpu.VMEM((1, LANES), f32),
            pltpu.VMEM((3, 1, LANES), f32),
            pltpu.VMEM((1, LANES), f32),
            pltpu.VMEM((shards - 1, 1, LANES), f32),
            dma((2,)),
            dma,
            dma,
            dma((2,)),
            regular,
            regular,
            dma,
            dma((len(pieces(0, chunks)), 2)),
            dma,
            dma((chunks // 2,)),
            dma,
            dma((len(pieces(0, chunks)),)),
            dma,
            dma,
            dma,
            dma,
            dma,
            dma,
            dma,
            dma,
            dma,
            dma,
            dma,
            dma,
            dma,
            dma,
            dma,
        ],
        compiler_params=pltpu.CompilerParams(
            collective_id=0,
            has_side_effects=True,
            vmem_limit_bytes=57 * 1024 * 1024,
        ),
    )(x.reshape(4 * chunks, PART, cols), joined, slot)
    return pl.pallas_call(
        functools.partial(store_kernel, slots_dev),
        out_shape=[
            jax.ShapeDtypeStruct((slots_dev, shards, rows, width), f32),
            jax.ShapeDtypeStruct((slots_dev,), f32),
            jax.ShapeDtypeStruct((3,), f32),
        ],
        in_specs=[pl.BlockSpec(memory_space=pltpu.VMEM)] * 4,
        out_specs=[pl.BlockSpec(memory_space=pltpu.HBM)] * 3,
        scratch_shapes=[
            pltpu.VMEM((slots_dev, shards, LATE * PART, width), f32),
            pltpu.SMEM((slots_dev,), f32),
            pltpu.SMEM((3,), f32),
            dma((3,)),
        ],
        compiler_params=pltpu.CompilerParams(vmem_limit_bytes=4 * 1024 * 1024),
    )(out, late, total, kinds)


def any_kernel(groups, shards, blocks, slots_dev, chunks, *refs):
    x_ref, joined_ref, slot_ref = refs[:3]
    out_ref, head_ref, type_ref = refs[3:6]
    own = refs[6]
    got = refs[7 : 7 + chunks]
    ready = refs[7 + chunks : 7 + 2 * chunks]
    rest = refs[7 + 2 * chunks :]
    (source, taken, kind_of, summed, squares, shard_part, shard_all, grp_part, grp_all) = rest[:9]
    (own_sem, z_send, z_recv, a_send, a_recv, keep_sem, s_send, s_recv, g_send, g_recv) = rest[9:]

    grp = lax.axis_index("grp")
    shard = lax.axis_index("shard")
    slots = slots_dev * shards
    rows = own.shape[0]
    part = rows // chunks
    width = own.shape[1] // blocks

    def grp_peer(offset):
        return lax.rem(grp + offset, groups)

    def shard_peer(offset):
        return lax.rem(shard + offset, shards)

    load_own = pltpu.make_async_copy(
        x_ref.at[0, pl.ds(pl.multiple_of(grp * rows, 8), rows), :], own, own_sem
    )
    load_own.start()

    barrier = pltpu.get_barrier_semaphore()
    for o in range(1, groups):
        pl.semaphore_signal(barrier, 1, device_id=(grp_peer(o), shard), device_id_type=MESH)
    for o in range(1, shards):
        pl.semaphore_signal(barrier, 1, device_id=(grp, shard_peer(o)), device_id_type=MESH)
    pl.semaphore_wait(barrier, groups + shards - 2)

    z_copies = []
    for c in range(chunks):
        for o in range(1, groups):
            first = pl.multiple_of(grp_peer(o) * rows + c * part, 8)
            copy = pltpu.make_async_remote_copy(
                src_ref=x_ref.at[0, pl.ds(first, part), :],
                dst_ref=got[c].at[o - 1],
                send_sem=z_send.at[c, o - 1],
                recv_sem=z_recv.at[c, o - 1],
                device_id=(grp_peer(o), shard),
                device_id_type=MESH,
            )
            copy.start()
            z_copies.append(copy)

    def find(j, carry):
        found, block, kind = jnp.float32(0), jnp.int32(0), jnp.int32(3)
        for b in range(blocks):
            hit = slot_ref[b] == j
            found = jnp.where(hit, 1.0, found)
            block = jnp.where(hit, joined_ref[b], block)
            kind = jnp.where(hit, (b >= QH) + (b >= QH + KVH), kind)
        source[j] = block
        taken[j] = found
        kind_of[j] = kind
        return carry

    lax.fori_loop(0, slots, find, 0)

    load_own.wait()
    a_copies = []
    for c in range(chunks):
        for o in range(1, groups):
            z_copies[c * (groups - 1) + o - 1].wait_recv()

        def add(k, carry):
            at = pl.multiple_of(k * width, width)
            total = own[c * part : (c + 1) * part, pl.ds(at, width)].astype(jnp.float32)
            for o in range(1, groups):
                total += got[c][o - 1, :, pl.ds(at, width)].astype(jnp.float32)
            summed[k] = total
            return carry

        lax.fori_loop(0, blocks, add, 0, unroll=4)

        def slot(j, carry):
            total = summed[source[j]] * taken[j]
            ready[c][j] = total
            sq = jnp.sum((total * total).reshape(part // 8, 8, width), axis=0)
            squares[j] = sq if c == 0 else squares[j] + sq
            return carry

        lax.fori_loop(0, slots, slot, 0, unroll=4)

        if c == chunks - 1:
            lane = lax.broadcasted_iota(jnp.int32, (slots, LANES), 1)
            row = lax.broadcasted_iota(jnp.int32, (slots, LANES), 0)
            per_slot = jnp.sum(jnp.sum(squares[...], axis=1), axis=1, keepdims=True)
            shard_part[...] = jnp.sum(jnp.where(lane == row, per_slot, 0.0), axis=0, keepdims=True)
            s_copies = []
            for o in range(1, shards):
                copy = pltpu.make_async_remote_copy(
                    src_ref=shard_part,
                    dst_ref=shard_all.at[o - 1],
                    send_sem=s_send.at[o - 1],
                    recv_sem=s_recv.at[o - 1],
                    device_id=(grp, shard_peer(o)),
                    device_id_type=MESH,
                )
                copy.start()
                s_copies.append(copy)

        for o in range(1, shards):
            copy = pltpu.make_async_remote_copy(
                src_ref=ready[c].at[pl.ds(shard_peer(o) * slots_dev, slots_dev)],
                dst_ref=out_ref.at[:, shard, pl.ds(c * part, part), :],
                send_sem=a_send.at[c, o - 1],
                recv_sem=a_recv.at[c, o - 1],
                device_id=(grp, shard_peer(o)),
                device_id_type=MESH,
            )
            copy.start()
            a_copies.append(copy)
        copy = pltpu.make_async_copy(
            ready[c].at[pl.ds(shard * slots_dev, slots_dev)],
            out_ref.at[:, shard, pl.ds(c * part, part), :],
            keep_sem.at[c],
        )
        copy.start()
        a_copies.append(copy)

    total = shard_part[...]
    for o in range(1, shards):
        s_copies[o - 1].wait()
        total = total + shard_all[o - 1]
    grp_part[...] = total
    g_copies = []
    for o in range(1, groups):
        copy = pltpu.make_async_remote_copy(
            src_ref=grp_part,
            dst_ref=grp_all.at[o - 1],
            send_sem=g_send.at[o - 1],
            recv_sem=g_recv.at[o - 1],
            device_id=(grp_peer(o), shard),
            device_id_type=MESH,
        )
        copy.start()
        g_copies.append(copy)
    lane = lax.broadcasted_iota(jnp.int32, (1, LANES), 1)

    def lay(j, kinds):
        return jnp.where(lane == j, kind_of[j], kinds)

    kinds = lax.fori_loop(0, slots, lay, jnp.full((1, LANES), 3, jnp.int32))
    for o in range(1, groups):
        g_copies[o - 1].wait()
        total = total + grp_all[o - 1]
    root = jnp.sqrt(total / (D * HS))
    for i in range(slots_dev):
        head_ref[i] = jnp.sum(jnp.where(lane == shard * slots_dev + i, root, 0.0))
    for t, heads in enumerate((QH, KVH, KVH)):
        one = jnp.sum(jnp.where(kinds == t, total, 0.0), axis=1, keepdims=True)
        type_ref[t] = jnp.sum(jnp.sqrt(one / (heads * D * HS)))

    for copy in z_copies:
        copy.wait_send()
    for copy in a_copies:
        copy.wait()


def any_step(x, joined, slot, groups, shards, blocks, slots_dev, rows, width):
    slots = slots_dev * shards
    cols = blocks * width
    part = chunk_rows(rows)
    chunks = rows // part
    dma = pltpu.SemaphoreType.DMA
    return pl.pallas_call(
        functools.partial(any_kernel, groups, shards, blocks, slots_dev, chunks),
        out_shape=[
            jax.ShapeDtypeStruct((slots_dev, shards, rows, width), jnp.float32),
            jax.ShapeDtypeStruct((slots_dev,), jnp.float32),
            jax.ShapeDtypeStruct((3,), jnp.float32),
        ],
        in_specs=[
            pl.BlockSpec(memory_space=pltpu.HBM),
            pl.BlockSpec(memory_space=pltpu.SMEM),
            pl.BlockSpec(memory_space=pltpu.SMEM),
        ],
        out_specs=[
            pl.BlockSpec(memory_space=pl.ANY),
            pl.BlockSpec(memory_space=pltpu.SMEM),
            pl.BlockSpec(memory_space=pltpu.SMEM),
        ],
        scratch_shapes=[pltpu.VMEM((rows, cols), jnp.bfloat16)]
        + [pltpu.VMEM((groups - 1, part, cols), jnp.bfloat16)] * chunks
        + [pltpu.VMEM((slots, part, width), jnp.float32)] * chunks
        + [
            pltpu.SMEM((slots,), jnp.int32),
            pltpu.SMEM((slots,), jnp.float32),
            pltpu.SMEM((slots,), jnp.int32),
            pltpu.VMEM((blocks, part, width), jnp.float32),
            pltpu.VMEM((slots, 8, width), jnp.float32),
            pltpu.VMEM((1, LANES), jnp.float32),
            pltpu.VMEM((shards - 1, 1, LANES), jnp.float32),
            pltpu.VMEM((1, LANES), jnp.float32),
            pltpu.VMEM((groups - 1, 1, LANES), jnp.float32),
            dma,
            dma((chunks, groups - 1)),
            dma((chunks, groups - 1)),
            dma((chunks, shards - 1)),
            dma((chunks, shards - 1)),
            dma((chunks,)),
            dma((shards - 1,)),
            dma((shards - 1,)),
            dma((groups - 1,)),
            dma((groups - 1,)),
        ],
        compiler_params=pltpu.CompilerParams(
            collective_id=0,
            has_side_effects=True,
            vmem_limit_bytes=60 * 1024 * 1024,
        ),
    )(x, joined, slot)


def solution(mesh):
    groups, shards = mesh.shape["grp"], mesh.shape["shard"]

    def step(x, joined, slot):
        blocks = joined.shape[0]
        slots_dev = (blocks + shards - 1) // shards
        rows = x.shape[1] // groups
        width = x.shape[2] // blocks
        line = groups == 4 and shards == 8 and rows == 16 * PART and blocks % GROUP == 0
        if line and width == LANES and slots_dev * shards <= LANES:
            return tuple(line_step(x, joined, slot, blocks, slots_dev, shards, rows, width))
        return tuple(any_step(x, joined, slot, groups, shards, blocks, slots_dev, rows, width))

    return jax.shard_map(
        step,
        mesh=mesh,
        in_specs=(P("grp", "shard", None), P(), P()),
        out_specs=(P("shard", None, "grp", None), P("shard"), P()),
        check_vma=False,
    )
```

```python
import functools

import jax
import jax.numpy as jnp
from jax import lax
from jax.experimental import pallas as pl
from jax.experimental.pallas import tpu as pltpu
from jax.sharding import PartitionSpec as P

D = 4096
QH = 32
KVH = 8
HS = 128
LANES = 128
MESH = pl.DeviceIdType.MESH


def chunk_rows(rows):
    return 16 if rows % 16 == 0 else rows


PART = 8
GROUP = 8
BITS = 19
QMAX = (1 - 2.0**-10) * 2.0 ** (BITS - 2)
SMALL = 2.0**-120
LATE = 5
LATE_COPIES = ((0, 1), (1, 2), (3, 2))
SINGLE = 2
PLAN = (("FNFNLfnLflnfnLMfAnm", 1), ("fnm", 3), ("m", 1))
AHEAD = 4


def pieces(first, last):
    c, found = first, []
    while c < last:
        n = 2 if c % 2 == 0 and c + 2 <= last and c >= SINGLE else 1
        found.append((c, n))
        c += n
    return found


def powers(e):
    half = e >> 1
    return jnp.exp2(half.astype(jnp.float32)), jnp.exp2((e - half).astype(jnp.float32))


def encode(tiles):
    peak = functools.reduce(jnp.maximum, [jnp.abs(t) for t in tiles])
    e = jnp.ceil(jnp.log2(jnp.maximum(peak, SMALL))).astype(jnp.int32) - 1
    p, q = powers(-e)
    p = p * QMAX
    codes = [jnp.round(t * q * p).astype(jnp.int32) for t in tiles]
    half, low = GROUP // 2, 32 - BITS
    high = BITS - low
    words = [(codes[i] << low) | (codes[half + i] & ((1 << low) - 1)) for i in range(half)]
    last = e << 24
    for i in range(half):
        last |= ((codes[half + i] >> low) & ((1 << high) - 1)) << (high * i)
    return words + [last]


def decode(words):
    half, low = GROUP // 2, 32 - BITS
    high = BITS - low
    p, q = powers(words[half] >> 24)
    p = p * (1.0 / QMAX)
    codes = [words[i] >> low for i in range(half)]
    for i in range(half):
        top = (words[half] << (32 - high * (i + 1))) >> (32 - high)
        codes.append((top << low) | (words[i] & ((1 << low) - 1)))
    return [c.astype(jnp.float32) * p * q for c in codes]


def piece(c, n):
    return c if n == 1 else lax.div(c, 2) + SINGLE // 2


def wait_for(ref, sem):
    pltpu.make_async_copy(ref, ref, sem).wait()


def steps(pattern, done):
    per = {k: sum(1 + c.islower() for c in pattern if c.lower() == k) for k in done}
    return dict(done), per


def flip(s, o):
    for b in range(3):
        if o >> b & 1:
            s = s + (1 - 2 * lax.rem(lax.div(s, 1 << b), 2)) * (1 << b)
    return s


def line_kernel(
    blocks,
    slots_dev,
    x_ref,
    joined_hbm,
    slot_hbm,
    out_ref,
    late_raw,
    total_ref,
    kinds_ref,
    joined_ref,
    slot_ref,
    first,
    own,
    far,
    passed,
    got,
    out_words,
    in_words,
    ready,
    late_src,
    late_mine,
    late_in,
    late_words,
    back_words,
    source,
    taken,
    kind_of,
    summed,
    squares,
    grp_part,
    grp_all,
    shard_part,
    shard_all,
    index_sem,
    first_sem,
    own_sem,
    far_sem,
    plane_sem,
    peers_sem,
    beyond_sem,
    r_send,
    r_recv,
    m_send,
    m_recv,
    w_send,
    w_recv,
    a_send,
    a_recv,
    a_late,
    g_send,
    g_recv,
    s_send,
    s_recv,
    late_sem,
    lx_send,
    lx_recv,
    lk_sem,
    lf_send,
    lf_recv,
    la_send,
    la_recv,
):
    groups, shards = 4, 8
    grp = lax.axis_index("grp")
    shard = lax.axis_index("shard")
    slots = slots_dev * shards
    chunks = own.shape[0]
    width = own.shape[2] // blocks
    sets = blocks // GROUP
    span = GROUP * width

    outer = (grp == 0) | (grp == groups - 1)
    inner = jnp.logical_not(outer)
    mate = grp + 1 - 2 * lax.rem(grp, 2)
    near = jnp.where(outer, 3 - mate, 3 - grp)
    beyond = near + 1 - 2 * lax.rem(near, 2)
    dests = (near, beyond)

    own_copy = pltpu.make_async_copy(x_ref.at[pl.ds(grp * chunks, chunks)], own, own_sem)

    def far_copy(f):
        return pltpu.make_async_copy(
            x_ref.at[pl.ds(dests[f] * chunks, chunks)], far.at[f], far_sem.at[f]
        )

    def send(src, dst, send_sem, recv_sem, to):
        return pltpu.make_async_remote_copy(
            src_ref=src,
            dst_ref=dst,
            send_sem=send_sem,
            recv_sem=recv_sem,
            device_id=to,
            device_id_type=MESH,
        )

    index_copies = [
        pltpu.make_async_copy(joined_hbm, joined_ref, index_sem.at[0]),
        pltpu.make_async_copy(slot_hbm, slot_ref, index_sem.at[1]),
    ]
    first_copy = pltpu.make_async_copy(x_ref.at[pl.ds(beyond * chunks, 1)], first, first_sem)

    def relay_copy(c, n, f):
        staged = isinstance(c, int) and c == 0 and f == 1
        src = first if staged else x_ref.at[pl.ds(dests[f] * chunks + c, n)]
        dst = passed.at[f, pl.ds(c, n)]
        return send(src, dst, r_send, r_recv.at[piece(c, n), f], (mate, shard))

    def mate_copy(c, n):
        src = x_ref.at[pl.ds(mate * chunks + c, n)]
        return send(src, got.at[pl.ds(c, n)], m_send, m_recv.at[lax.div(c, 2)], (mate, shard))

    def coded_copy(c, n, f):
        at = pl.ds(c, n)
        to = (dests[f], shard)
        return send(out_words.at[f, at], in_words.at[at], w_send, w_recv.at[piece(c, n)], to)

    order = (6, 7, 2, 4, 3, 5, 1)

    def rows_of(c, n):
        return pl.ds(pl.multiple_of(c * PART, PART), n * PART)

    def rows_copy(c, n, o, recv_sem):
        to = flip(shard, o)
        return send(
            ready.at[pl.ds(to * slots_dev, slots_dev), rows_of(c, n)],
            out_ref.at[:, shard, rows_of(c, n), :],
            a_send,
            recv_sem,
            (grp, to),
        )

    def others(first, last):
        at = pl.ds(first * PART, (last - first) * PART)
        return ready.at[pl.ds(0, (shards - 1) * slots_dev), at]

    late_copy = pltpu.make_async_copy(x_ref.at[pl.ds(mate * chunks, LATE)], late_src, late_sem)

    def swap_copy(o):
        to = flip(shard, o)
        return send(
            late_mine.at[:, pl.ds(to * slots_dev, slots_dev)],
            late_in.at[shard],
            lx_send,
            lx_recv,
            (grp, to),
        )

    stay_copy = pltpu.make_async_copy(
        late_mine.at[:, pl.ds(shard * slots_dev, slots_dev)], late_in.at[shard], lk_sem
    )

    def forward_copy(i):
        at = pl.ds(*LATE_COPIES[i])
        to = (mate, shard)
        return send(late_in.at[:, at], late_raw.at[:, at], lf_send, lf_recv, to)

    back_copy = send(late_words, back_words, la_send, la_recv, (mate, shard))

    first_copy.start()

    barrier = pltpu.get_barrier_semaphore()
    pl.semaphore_signal(barrier, 1, device_id=(mate, shard), device_id_type=MESH)

    @pl.when(inner)
    def _():
        for o in range(1, 6):
            to = (grp, flip(shard, o))
            pl.semaphore_signal(barrier, 1, device_id=to, device_id_type=MESH)
        pl.semaphore_signal(barrier, 1, device_id=(near, shard), device_id_type=MESH)
        pl.semaphore_wait(barrier, 7)
        to = (grp, flip(shard, 2))
        pl.semaphore_signal(plane_sem, 1, device_id=to, device_id_type=MESH)
        own_copy.start()
        pl.semaphore_signal(beyond_sem, 1, device_id=(near, shard), device_id_type=MESH)
        for f in range(2):
            far_copy(f).start()
        for c in range(0, AHEAD, 2):
            mate_copy(c, 2).start()

    @pl.when(outer)
    def _():
        pl.semaphore_wait(barrier, 1)
        first_copy.wait()
        done = dict(n=0, f=0, m=LATE)
        for pattern, times in PLAN:
            now, per = steps(pattern, done)

            def queue(k, carry, pattern=pattern, now=now, per=per):
                at = {key: now[key] + k * per[key] for key in now}
                for kind in pattern:
                    n, key = 1 + kind.islower(), kind.lower()
                    if key in "nf":
                        relay_copy(at[key], n, "nf".index(key)).start()
                    elif key == "m":
                        mate_copy(at[key], n).start()
                    if key in at:
                        at[key] += n
                return carry

            if times == 1:
                queue(0, 0)
            else:
                lax.fori_loop(0, times, queue, 0)
            done = {key: now[key] + times * per[key] for key in now}
        own_copy.start()
        late_copy.start()

    def find(j, carry):
        head = jnp.int32(-1)
        for b in range(blocks):
            head = jnp.where(slot_ref[b] == j, b, head)
        there = head >= 0
        source[j] = jnp.where(there, joined_ref[jnp.maximum(head, 0)], 0)
        taken[j] = jnp.where(there, 1.0, 0.0)
        kind = jnp.where(head >= QH, 1, 0) + jnp.where(head >= QH + KVH, 1, 0)
        kind_of[j] = jnp.where(there, kind, 3)
        return carry

    for copy in index_copies:
        copy.start()
    for copy in index_copies:
        copy.wait()

    @pl.when(inner)
    def _():
        pl.semaphore_wait(plane_sem, 1)
        for o in order:
            to = (grp, flip(shard, o))
            pl.semaphore_signal(peers_sem, 1, device_id=to, device_id_type=MESH)

    lax.fori_loop(0, slots, find, 0)

    @pl.when(inner)
    def _():
        pl.semaphore_wait(peers_sem, shards - 1)
        pl.semaphore_signal(plane_sem, 1, device_id=(mate, shard), device_id_type=MESH)

    own_copy.wait()

    def clear(j, carry):
        squares[j] = jnp.zeros((PART, width), jnp.float32)
        return carry

    lax.fori_loop(0, slots, clear, 0)

    def pack(c, n, f):
        relay_copy(c, n, f).wait_recv()

        def pack_set(q, carry):
            i, p = lax.div(q, sets), lax.rem(q, sets)
            at = pl.ds(pl.multiple_of(p * span, span), span)
            total = far[f, c + i, :, at].astype(jnp.float32)
            total += passed[f, c + i, :, at].astype(jnp.float32)
            words = encode([total[:, i * width : (i + 1) * width] for i in range(GROUP)])
            for w, word in enumerate(words):
                out_words[f, c + i, p, w] = word
            return carry

        lax.fori_loop(0, n * sets, pack_set, 0, unroll=2)
        coded_copy(c, n, f).start()
        if f == 1 and n == 2:

            @pl.when(c + AHEAD - SINGLE < chunks)
            def _():
                mate_copy(c + AHEAD - SINGLE, 2).start()

    def wait_coded(c, n):
        coded_copy(c, n, 0).wait_recv()

    def finish(c, n, arrive):
        for i in range(n):

            def pre_set(p, carry, i=i):
                at = pl.ds(pl.multiple_of(p * span, span), span)
                mine = own[c + i, :, at].astype(jnp.float32)
                words = [in_words[c + i, p, w] for w in range(GROUP // 2 + 1)]
                for t, tile in enumerate(decode(words)):
                    summed[i, p * GROUP + t] = mine[:, t * width : (t + 1) * width] + tile
                return carry

            lax.fori_loop(0, sets, pre_set, 0, unroll=2)
        if arrive is not None:
            arrive()
        for i in range(n):

            def add_set(p, carry, i=i):
                at = pl.ds(pl.multiple_of(p * span, span), span)
                more = got[c + i, :, at].astype(jnp.float32)
                for t in range(GROUP):
                    summed[i, p * GROUP + t] += more[:, t * width : (t + 1) * width]
                return carry

            if arrive is not None:
                lax.fori_loop(0, sets, add_set, 0, unroll=2)

            def place(j, carry, i=i):
                total = summed[i, source[j]] * taken[j]
                ready[j, rows_of(c + i, 1)] = total
                if arrive is not None:
                    squares[j] += total * total
                return carry

            lax.fori_loop(0, slots, place, 0, unroll=8)
        for o in order:
            rows_copy(c, n, o, a_late if arrive is None else a_recv).start()
        mine = ready[pl.ds(shard * slots_dev, slots_dev), rows_of(c, n)]
        out_ref[:, shard, rows_of(c, n), :] = mine

    def late_chunk(c, n):
        if c < SINGLE or c % 2 == 0:
            wait_coded(c, 1 if c < SINGLE else 2)
        finish(c, n, None)

    def own_chunk(c, n):
        if n == 2:
            wait_coded(c, n)
        finish(c, n, lambda: mate_copy(c, n).wait_recv())

    def tell(j, carry):
        for n in range(LATE):
            at = pl.ds(n * PART, PART)
            words = encode([out_ref[j, a, at, :] for a in range(shards)])
            for i, word in enumerate(words):
                late_words[n, j, i] = word
        return carry

    @pl.when(inner)
    def _():
        first_copy.wait()
        for f in range(2):
            far_copy(f).wait()
        pl.semaphore_wait(beyond_sem, 1)
        done = dict(n=0, f=0, l=0, m=LATE)
        for pattern, times in PLAN:
            now, per = steps(pattern, done)

            def act(k, carry, pattern=pattern, now=now, per=per):
                at = {key: now[key] + k * per[key] for key in now}
                for kind in pattern:
                    n, key = 1 + kind.islower(), kind.lower()
                    if key in "nf":
                        pack(at[key], n, "nf".index(key))
                    elif key == "m":
                        own_chunk(at[key], n)
                    elif key == "l":
                        late_chunk(at[key], n)
                    else:
                        wait_for(others(0, LATE), a_late)
                        lax.fori_loop(0, slots_dev, tell, 0)
                        back_copy.start()
                    if key in at:
                        at[key] += n
                return carry

            if times == 1:
                act(0, 0)
            else:
                lax.fori_loop(0, times, act, 0)
            done = {key: now[key] + times * per[key] for key in now}
    @pl.when(outer)
    def _():
        pl.semaphore_wait(plane_sem, 1)
        late_copy.wait()

        for n in range(LATE):

            def split(p, carry, n=n):
                at = pl.ds(pl.multiple_of(p * span, span), span)
                rows = late_src[n, :, at].astype(jnp.float32)
                for i in range(GROUP):
                    summed[0, p * GROUP + i] = rows[:, i * width : (i + 1) * width]
                return carry

            lax.fori_loop(0, sets, split, 0, unroll=2)

            def arrange(j, carry, n=n):
                late_mine[n, j] = (summed[0, source[j]] * taken[j]).astype(jnp.bfloat16)
                return carry

            lax.fori_loop(0, slots, arrange, 0, unroll=4)
        for o in order:
            swap_copy(o).start()
        stay_copy.start()
        stay_copy.wait()
        wait_for(late_in.at[pl.ds(0, shards - 1)], lx_recv)
        forward_copy(0).start()

        def own_pair(k, carry):
            c = 2 * k
            finish(c, 2, lambda: mate_copy(c, 2).wait_recv())
            return carry

        def coded_pair(k, carry):
            wait_coded(2 * k, 2)
            return own_pair(k, carry)

        for c, n in pieces(0, 2):
            wait_coded(c, n)
        own_pair(0, 0)
        lax.fori_loop(1, chunks // 2 - 2, coded_pair, 0)
        back_copy.wait_recv()

        def late_squares(j, carry):
            acc = jnp.zeros((PART, width), jnp.float32)
            for n in range(LATE):
                tiles = decode([back_words[n, j, i] for i in range(GROUP // 2 + 1)])
                for a, tile in enumerate(tiles):
                    total = tile + late_in[a, n, j].astype(jnp.float32)
                    acc += total * total
            squares[shard * slots_dev + j] += acc
            return carry

        lax.fori_loop(0, slots_dev, late_squares, 0)
        lax.fori_loop(chunks // 2 - 2, chunks // 2, coded_pair, 0)

    lane = lax.broadcasted_iota(jnp.int32, (slots, LANES), 1)
    row = lax.broadcasted_iota(jnp.int32, (slots, LANES), 0)
    per_slot = jnp.sum(jnp.sum(squares[...], axis=1), axis=1, keepdims=True)
    total = jnp.sum(jnp.where(lane == row, per_slot, 0.0), axis=0, keepdims=True)

    def grp_copy(o):
        to = lax.rem(grp + o, groups)
        return send(grp_part, grp_all.at[o - 1], g_send, g_recv, (to, shard))

    def shard_copy(o):
        to = flip(shard, o)
        return send(
            shard_part, shard_all.at[o - 1], s_send, s_recv, (grp, to)
        )

    grp_part[...] = total
    for o in range(1, groups):
        grp_copy(o).start()

    @pl.when(outer)
    def _():
        for i in range(1, len(LATE_COPIES)):
            forward_copy(i).start()

    lane = lax.broadcasted_iota(jnp.int32, (1, LANES), 1)

    def lay(j, kinds):
        return jnp.where(lane == j, kind_of[j], kinds)

    kinds = lax.fori_loop(0, slots, lay, jnp.full((1, LANES), 3, jnp.int32))

    wait_for(grp_all, g_recv)
    for o in range(1, groups):
        total = total + grp_all[o - 1]
    shard_part[...] = total
    for o in order:
        shard_copy(o).start()

    @pl.when(inner)
    def _():
        wait_for(out_words, w_send)
        wait_for(got, m_send)
        back_copy.wait_send()
        wait_for(others(LATE, chunks), a_recv)

    @pl.when(outer)
    def _():
        wait_for(passed, r_send)
        wait_for(got.at[pl.ds(LATE, chunks - LATE)], m_send)
        wait_for(late_in.at[pl.ds(0, shards - 1)], lx_send)
        wait_for(others(0, chunks), a_recv)

    wait_for(others(0, chunks), a_send)
    wait_for(grp_all, g_send)
    wait_for(shard_all, s_recv)
    wait_for(shard_all, s_send)
    for o in order:
        total = total + shard_all[o - 1]
    total_ref[...] = total
    kinds_ref[...] = kinds

    @pl.when(outer)
    def _():
        wait_for(late_in, lf_send)

    @pl.when(inner)
    def _():
        wait_for(late_raw, lf_recv)


def store_kernel(
    slots_dev,
    in_ref,
    late_ref,
    total_ref,
    kinds_ref,
    out_ref,
    head_ref,
    type_ref,
    late_out,
    heads,
    types,
    sems,
):
    shards = in_ref.shape[1]
    late = pl.ds(0, LATE * PART)
    rest = pl.ds(LATE * PART, in_ref.shape[2] - LATE * PART)
    bulk = [
        pltpu.make_async_copy(in_ref.at[j, :, rest], out_ref.at[j, :, rest], sems.at[0])
        for j in range(slots_dev)
    ]
    tops = [
        pltpu.make_async_copy(late_out.at[j], out_ref.at[j, :, late], sems.at[0])
        for j in range(slots_dev)
    ]
    small = [
        pltpu.make_async_copy(heads, head_ref, sems.at[1]),
        pltpu.make_async_copy(types, type_ref, sems.at[2]),
    ]
    for copy in bulk:
        copy.start()
    grp, shard = lax.axis_index("grp"), lax.axis_index("shard")
    inner = (grp > 0) & (grp < lax.axis_size("grp") - 1)
    for j in range(slots_dev):

        def add_late(a, carry, j=j):
            for c in range(LATE):
                at = pl.ds(c * PART, PART)
                more = jnp.where(inner, late_ref[a, c, j].astype(jnp.float32), 0.0)
                late_out[j, a, at, :] = in_ref[j, a, at, :] + more
            return carry

        lax.fori_loop(0, shards, add_late, 0, unroll=True)
        tops[j].start()
    total = total_ref[...]
    kinds = kinds_ref[...]
    lane = lax.broadcasted_iota(jnp.int32, (1, LANES), 1)
    root = jnp.sqrt(total / (D * HS))
    for i in range(slots_dev):
        heads[i] = jnp.sum(jnp.where(lane == shard * slots_dev + i, root, 0.0))
    for t, count in enumerate((QH, KVH, KVH)):
        one = jnp.sum(jnp.where(kinds == t, total, 0.0), axis=1, keepdims=True)
        types[t] = jnp.sum(jnp.sqrt(one / (count * D * HS)))
    for copy in small:
        copy.start()
    for copy in small:
        copy.wait()
    wait_for(out_ref, sems.at[0])


def line_step(x, joined, slot, blocks, slots_dev, shards, rows, width):
    chunks = rows // PART
    cols = blocks * width
    sets = blocks // GROUP
    slots = slots_dev * shards
    half = GROUP // 2
    dma = pltpu.SemaphoreType.DMA
    regular = pltpu.SemaphoreType.REGULAR
    f32, i32, bf16 = jnp.float32, jnp.int32, jnp.bfloat16
    out, late, total, kinds = pl.pallas_call(
        functools.partial(line_kernel, blocks, slots_dev),
        out_shape=[
            pltpu.VMEM((slots_dev, shards, rows, width), f32),
            pltpu.VMEM((shards, LATE, slots_dev, PART, width), bf16),
            pltpu.VMEM((1, LANES), f32),
            pltpu.VMEM((1, LANES), i32),
        ],
        in_specs=[pl.BlockSpec(memory_space=pltpu.HBM)] * 3,
        out_specs=[pl.BlockSpec(memory_space=pltpu.VMEM)] * 4,
        scratch_shapes=[
            pltpu.SMEM((blocks,), i32),
            pltpu.SMEM((blocks,), i32),
            pltpu.VMEM((1, PART, cols), bf16),
            pltpu.VMEM((chunks, PART, cols), bf16),
            pltpu.VMEM((2, chunks, PART, cols), bf16),
            pltpu.VMEM((2, chunks, PART, cols), bf16),
            pltpu.VMEM((chunks, PART, cols), bf16),
            pltpu.VMEM((2, chunks, sets, half + 1, PART, width), i32),
            pltpu.VMEM((chunks, sets, half + 1, PART, width), i32),
            pltpu.VMEM((slots, rows, width), f32),
            pltpu.VMEM((LATE, PART, cols), bf16),
            pltpu.VMEM((LATE, slots, PART, width), bf16),
            pltpu.VMEM((shards, LATE, slots_dev, PART, width), bf16),
            pltpu.VMEM((LATE, slots_dev, half + 1, PART, width), i32),
            pltpu.VMEM((LATE, slots_dev, half + 1, PART, width), i32),
            pltpu.SMEM((slots,), i32),
            pltpu.SMEM((slots,), f32),
            pltpu.SMEM((slots,), i32),
            pltpu.VMEM((2, blocks, PART, width), f32),
            pltpu.VMEM((slots, PART, width), f32),
            pltpu.VMEM((1, LANES), f32),
            pltpu.VMEM((3, 1, LANES), f32),
            pltpu.VMEM((1, LANES), f32),
            pltpu.VMEM((shards - 1, 1, LANES), f32),
            dma((2,)),
            dma,
            dma,
            dma((2,)),
            regular,
            regular,
            regular,
            dma,
            dma((len(pieces(0, chunks)), 2)),
            dma,
            dma((chunks // 2,)),
            dma,
            dma((len(pieces(0, chunks)),)),
            dma,
            dma,
            dma,
            dma,
            dma,
            dma,
            dma,
            dma,
            dma,
            dma,
            dma,
            dma,
            dma,
            dma,
            dma,
        ],
        compiler_params=pltpu.CompilerParams(
            collective_id=0,
            has_side_effects=True,
            vmem_limit_bytes=57 * 1024 * 1024,
        ),
    )(x.reshape(4 * chunks, PART, cols), joined, slot)
    return pl.pallas_call(
        functools.partial(store_kernel, slots_dev),
        out_shape=[
            jax.ShapeDtypeStruct((slots_dev, shards, rows, width), f32),
            jax.ShapeDtypeStruct((slots_dev,), f32),
            jax.ShapeDtypeStruct((3,), f32),
        ],
        in_specs=[pl.BlockSpec(memory_space=pltpu.VMEM)] * 4,
        out_specs=[pl.BlockSpec(memory_space=pltpu.HBM)] * 3,
        scratch_shapes=[
            pltpu.VMEM((slots_dev, shards, LATE * PART, width), f32),
            pltpu.SMEM((slots_dev,), f32),
            pltpu.SMEM((3,), f32),
            dma((3,)),
        ],
        compiler_params=pltpu.CompilerParams(vmem_limit_bytes=4 * 1024 * 1024),
    )(out, late, total, kinds)


def any_kernel(groups, shards, blocks, slots_dev, chunks, *refs):
    x_ref, joined_ref, slot_ref = refs[:3]
    out_ref, head_ref, type_ref = refs[3:6]
    own = refs[6]
    got = refs[7 : 7 + chunks]
    ready = refs[7 + chunks : 7 + 2 * chunks]
    rest = refs[7 + 2 * chunks :]
    (source, taken, kind_of, summed, squares, shard_part, shard_all, grp_part, grp_all) = rest[:9]
    (own_sem, z_send, z_recv, a_send, a_recv, keep_sem, s_send, s_recv, g_send, g_recv) = rest[9:]

    grp = lax.axis_index("grp")
    shard = lax.axis_index("shard")
    slots = slots_dev * shards
    rows = own.shape[0]
    part = rows // chunks
    width = own.shape[1] // blocks

    def grp_peer(offset):
        return lax.rem(grp + offset, groups)

    def shard_peer(offset):
        return lax.rem(shard + offset, shards)

    load_own = pltpu.make_async_copy(
        x_ref.at[0, pl.ds(pl.multiple_of(grp * rows, 8), rows), :], own, own_sem
    )
    load_own.start()

    barrier = pltpu.get_barrier_semaphore()
    for o in range(1, groups):
        pl.semaphore_signal(barrier, 1, device_id=(grp_peer(o), shard), device_id_type=MESH)
    for o in range(1, shards):
        pl.semaphore_signal(barrier, 1, device_id=(grp, shard_peer(o)), device_id_type=MESH)
    pl.semaphore_wait(barrier, groups + shards - 2)

    z_copies = []
    for c in range(chunks):
        for o in range(1, groups):
            first = pl.multiple_of(grp_peer(o) * rows + c * part, 8)
            copy = pltpu.make_async_remote_copy(
                src_ref=x_ref.at[0, pl.ds(first, part), :],
                dst_ref=got[c].at[o - 1],
                send_sem=z_send.at[c, o - 1],
                recv_sem=z_recv.at[c, o - 1],
                device_id=(grp_peer(o), shard),
                device_id_type=MESH,
            )
            copy.start()
            z_copies.append(copy)

    def find(j, carry):
        found, block, kind = jnp.float32(0), jnp.int32(0), jnp.int32(3)
        for b in range(blocks):
            hit = slot_ref[b] == j
            found = jnp.where(hit, 1.0, found)
            block = jnp.where(hit, joined_ref[b], block)
            kind = jnp.where(hit, (b >= QH) + (b >= QH + KVH), kind)
        source[j] = block
        taken[j] = found
        kind_of[j] = kind
        return carry

    lax.fori_loop(0, slots, find, 0)

    load_own.wait()
    a_copies = []
    for c in range(chunks):
        for o in range(1, groups):
            z_copies[c * (groups - 1) + o - 1].wait_recv()

        def add(k, carry):
            at = pl.multiple_of(k * width, width)
            total = own[c * part : (c + 1) * part, pl.ds(at, width)].astype(jnp.float32)
            for o in range(1, groups):
                total += got[c][o - 1, :, pl.ds(at, width)].astype(jnp.float32)
            summed[k] = total
            return carry

        lax.fori_loop(0, blocks, add, 0, unroll=4)

        def slot(j, carry):
            total = summed[source[j]] * taken[j]
            ready[c][j] = total
            sq = jnp.sum((total * total).reshape(part // 8, 8, width), axis=0)
            squares[j] = sq if c == 0 else squares[j] + sq
            return carry

        lax.fori_loop(0, slots, slot, 0, unroll=4)

        if c == chunks - 1:
            lane = lax.broadcasted_iota(jnp.int32, (slots, LANES), 1)
            row = lax.broadcasted_iota(jnp.int32, (slots, LANES), 0)
            per_slot = jnp.sum(jnp.sum(squares[...], axis=1), axis=1, keepdims=True)
            shard_part[...] = jnp.sum(jnp.where(lane == row, per_slot, 0.0), axis=0, keepdims=True)
            s_copies = []
            for o in range(1, shards):
                copy = pltpu.make_async_remote_copy(
                    src_ref=shard_part,
                    dst_ref=shard_all.at[o - 1],
                    send_sem=s_send.at[o - 1],
                    recv_sem=s_recv.at[o - 1],
                    device_id=(grp, shard_peer(o)),
                    device_id_type=MESH,
                )
                copy.start()
                s_copies.append(copy)

        for o in range(1, shards):
            copy = pltpu.make_async_remote_copy(
                src_ref=ready[c].at[pl.ds(shard_peer(o) * slots_dev, slots_dev)],
                dst_ref=out_ref.at[:, shard, pl.ds(c * part, part), :],
                send_sem=a_send.at[c, o - 1],
                recv_sem=a_recv.at[c, o - 1],
                device_id=(grp, shard_peer(o)),
                device_id_type=MESH,
            )
            copy.start()
            a_copies.append(copy)
        copy = pltpu.make_async_copy(
            ready[c].at[pl.ds(shard * slots_dev, slots_dev)],
            out_ref.at[:, shard, pl.ds(c * part, part), :],
            keep_sem.at[c],
        )
        copy.start()
        a_copies.append(copy)

    total = shard_part[...]
    for o in range(1, shards):
        s_copies[o - 1].wait()
        total = total + shard_all[o - 1]
    grp_part[...] = total
    g_copies = []
    for o in range(1, groups):
        copy = pltpu.make_async_remote_copy(
            src_ref=grp_part,
            dst_ref=grp_all.at[o - 1],
            send_sem=g_send.at[o - 1],
            recv_sem=g_recv.at[o - 1],
            device_id=(grp_peer(o), shard),
            device_id_type=MESH,
        )
        copy.start()
        g_copies.append(copy)
    lane = lax.broadcasted_iota(jnp.int32, (1, LANES), 1)

    def lay(j, kinds):
        return jnp.where(lane == j, kind_of[j], kinds)

    kinds = lax.fori_loop(0, slots, lay, jnp.full((1, LANES), 3, jnp.int32))
    for o in range(1, groups):
        g_copies[o - 1].wait()
        total = total + grp_all[o - 1]
    root = jnp.sqrt(total / (D * HS))
    for i in range(slots_dev):
        head_ref[i] = jnp.sum(jnp.where(lane == shard * slots_dev + i, root, 0.0))
    for t, heads in enumerate((QH, KVH, KVH)):
        one = jnp.sum(jnp.where(kinds == t, total, 0.0), axis=1, keepdims=True)
        type_ref[t] = jnp.sum(jnp.sqrt(one / (heads * D * HS)))

    for copy in z_copies:
        copy.wait_send()
    for copy in a_copies:
        copy.wait()


def any_step(x, joined, slot, groups, shards, blocks, slots_dev, rows, width):
    slots = slots_dev * shards
    cols = blocks * width
    part = chunk_rows(rows)
    chunks = rows // part
    dma = pltpu.SemaphoreType.DMA
    return pl.pallas_call(
        functools.partial(any_kernel, groups, shards, blocks, slots_dev, chunks),
        out_shape=[
            jax.ShapeDtypeStruct((slots_dev, shards, rows, width), jnp.float32),
            jax.ShapeDtypeStruct((slots_dev,), jnp.float32),
            jax.ShapeDtypeStruct((3,), jnp.float32),
        ],
        in_specs=[
            pl.BlockSpec(memory_space=pltpu.HBM),
            pl.BlockSpec(memory_space=pltpu.SMEM),
            pl.BlockSpec(memory_space=pltpu.SMEM),
        ],
        out_specs=[
            pl.BlockSpec(memory_space=pl.ANY),
            pl.BlockSpec(memory_space=pltpu.SMEM),
            pl.BlockSpec(memory_space=pltpu.SMEM),
        ],
        scratch_shapes=[pltpu.VMEM((rows, cols), jnp.bfloat16)]
        + [pltpu.VMEM((groups - 1, part, cols), jnp.bfloat16)] * chunks
        + [pltpu.VMEM((slots, part, width), jnp.float32)] * chunks
        + [
            pltpu.SMEM((slots,), jnp.int32),
            pltpu.SMEM((slots,), jnp.float32),
            pltpu.SMEM((slots,), jnp.int32),
            pltpu.VMEM((blocks, part, width), jnp.float32),
            pltpu.VMEM((slots, 8, width), jnp.float32),
            pltpu.VMEM((1, LANES), jnp.float32),
            pltpu.VMEM((shards - 1, 1, LANES), jnp.float32),
            pltpu.VMEM((1, LANES), jnp.float32),
            pltpu.VMEM((groups - 1, 1, LANES), jnp.float32),
            dma,
            dma((chunks, groups - 1)),
            dma((chunks, groups - 1)),
            dma((chunks, shards - 1)),
            dma((chunks, shards - 1)),
            dma((chunks,)),
            dma((shards - 1,)),
            dma((shards - 1,)),
            dma((groups - 1,)),
            dma((groups - 1,)),
        ],
        compiler_params=pltpu.CompilerParams(
            collective_id=0,
            has_side_effects=True,
            vmem_limit_bytes=60 * 1024 * 1024,
        ),
    )(x, joined, slot)


def solution(mesh):
    groups, shards = mesh.shape["grp"], mesh.shape["shard"]

    def step(x, joined, slot):
        blocks = joined.shape[0]
        slots_dev = (blocks + shards - 1) // shards
        rows = x.shape[1] // groups
        width = x.shape[2] // blocks
        line = groups == 4 and shards == 8 and rows == 16 * PART and blocks % GROUP == 0
        if line and width == LANES and slots_dev * shards <= LANES:
            return tuple(line_step(x, joined, slot, blocks, slots_dev, shards, rows, width))
        return tuple(any_step(x, joined, slot, groups, shards, blocks, slots_dev, rows, width))

    return jax.shard_map(
        step,
        mesh=mesh,
        in_specs=(P("grp", "shard", None), P(), P()),
        out_specs=(P("shard", None, "grp", None), P("shard"), P()),
        check_vma=False,
    )
```
